32 devices in a mesh: img: 4 (over x, core), tp: 8 (over z, y).
Axes of the slice: x: 2, y: 2, z: 4, core: 2. Of those that a mesh axis runs over, the one named last changes fastest.
Arguments:
- patch_tokens: bfloat16 [4096, 1024], P(('img', 'tp')), may hold values from -12 to 12
- norm_gain: float32 [1024], replicated, may hold values from 0.1 to 1.9
- norm_bias: float32 [1024], replicated, may hold values from -3 to 3
- up_weight: bfloat16 [1024, 8192], P('img', 'tp'), may hold values from -0.1875 to 0.1875
- up_bias: float32 [8192], P('tp'), may hold values from -3 to 3
- down_weight: bfloat16 [8192, 4096], P('tp', 'img'), may hold values from -0.125 to 0.125
- down_bias: float32 [4096], replicated, may hold values from -3 to 3
Outputs:
- projected: bfloat16 [4096, 4096], P(('img', 'tp'))
The draws below stay inside these ranges and needn't reach their ends.
All inputs are finite; a program needn't handle non-finite values.
Results may differ from the reference program's by a relative error of at most 0.014.
Values may be sent and summed in bfloat16 or wider, within the bound.
A program may use at most 128 MiB of HBM per device.

```python
import jax
import jax.numpy as jnp
from jax import lax

D = 1024
FF = 8192
DOUT = 4096
TOK_DEV = 128
TOKENS = 4096
N_IMG = 4
N_TP = 8


def level_of(own_key, dims, pieces, low, top_value):
    loudness = 1.0
    for axis_at, blocks in pieces:
        draws = jax.random.uniform(jax.random.fold_in(jax.random.fold_in(own_key, 6), axis_at), (blocks,), jnp.float32, low / len(pieces), top_value / len(pieces))
        loudness = loudness * jnp.repeat(jnp.exp(draws), dims[axis_at] // blocks).reshape((-1,) + (1,) * (len(dims) - 1 - axis_at))
    return loudness


def centred(rng, dims, width, reach, pieces=(), held_as=jnp.bfloat16):
    result = width * jax.random.normal(rng, dims, jnp.float32)
    if pieces:
        result = result * level_of(rng, dims, pieces, -0.22, 0.18)
    return jnp.clip(result, -reach, reach).astype(held_as)


def setup_inputs(seed: int = 0) -> dict:
    keys = jax.random.split(jax.random.key(seed), 8)
    patch_tokens = centred(keys[0], (TOKENS, D), 2.0, 12.0, ((0, 32),))
    norm_gain = jnp.clip(1.0 + 0.18 * jax.random.normal(keys[1], (D,), jnp.float32), 0.1, 1.9)
    norm_bias = centred(keys[2], (D,), 0.5, 3.0, (), jnp.float32)
    up_weight = centred(keys[3], (D, FF), D ** -0.5, 0.1875, ((0, 4), (1, 8)))
    up_bias = centred(keys[4], (FF,), 0.5, 3.0, ((0, 8),), jnp.float32)
    down_weight = centred(keys[5], (FF, DOUT), (FF // 4) ** -0.5, 0.125, ((0, 8), (1, 4)))
    down_bias = centred(keys[6], (DOUT,), 0.5, 3.0, (), jnp.float32)
    return dict(patch_tokens=patch_tokens, norm_gain=norm_gain, norm_bias=norm_bias, up_weight=up_weight, up_bias=up_bias, down_weight=down_weight, down_bias=down_bias)


def normalize(rows, norm_gain, norm_bias):
    values = rows.astype(jnp.float32)
    center = lax.optimization_barrier(jnp.mean(values, axis=1, keepdims=True))
    spread = lax.optimization_barrier(jnp.mean((values - center) ** 2, axis=1, keepdims=True))
    return ((values - center) * lax.rsqrt(spread + 1e-05) * norm_gain + norm_bias).astype(jnp.bfloat16)

def reference(patch_tokens, norm_gain, norm_bias, up_weight, up_bias, down_weight, down_bias):
    block_rows = TOK_DEV * N_TP
    group_width = FF // N_TP
    blocks = patch_tokens.reshape(N_IMG, block_rows, D)

    def one_block(rows):
        normed = normalize(rows, norm_gain, norm_bias)
        hidden = jax.nn.gelu(jnp.dot(normed, up_weight, preferred_element_type=jnp.float32) + up_bias).astype(jnp.bfloat16)

        def add_group(group, total):
            start = (group * group_width).astype(jnp.int32)
            cols = lax.dynamic_slice_in_dim(hidden, start, group_width, 1)
            weights = lax.dynamic_slice_in_dim(down_weight, start, group_width, 0)
            partial_value = jnp.dot(cols, weights, preferred_element_type=jnp.float32).astype(jnp.bfloat16)
            partial_value = lax.optimization_barrier(partial_value)
            return total + partial_value.astype(jnp.float32)
        total = lax.fori_loop(0, N_TP, add_group, jnp.zeros((block_rows, DOUT), jnp.float32))
        return (total + down_bias).astype(jnp.bfloat16)
    return lax.map(one_block, blocks).reshape(TOKENS, DOUT)
```

```python
import functools

import jax
import jax.numpy as jnp
from jax import lax
from jax.experimental import pallas as pl
from jax.experimental.pallas import tpu as pltpu
from jax.sharding import PartitionSpec as P

MESH = pl.DeviceIdType.MESH
LANES = 128
UP_STAGES = 2
LAG = 2
TILE = 256


def portion(size, num, den):
    return max(size * num // den // 16 * 16, 16)


def kernel(n_img, n_tp, x_hbm, gain_hbm, nbias_hbm, up_hbm, ubias_hbm, down_hbm, dbias_hbm, out_hbm,
           xv, gain, nbias, ubias, dbias, tok, normed, upf, ubf, hidden, dn, pb, from_low, from_high, ov,
           in_sem, own_sem, out_sem, tu_s, tu_r, td_s, td_r, bs_s, bs_r,
           dx_s, dx_r, dm_s, dm_r, r1_s, r1_r, r2_s, r2_r, p_s, p_r, lo_s, lo_r, hi_s, hi_r):
    cores = 2 if n_img % 2 == 0 else 1
    pair = 2 if n_tp % 2 == 0 else 1
    n_x, n_g = n_img // cores, n_tp // pair
    img, tp = lax.axis_index("img"), lax.axis_index("tp")
    x, c = img // cores, img % cores
    g, m = tp // pair, tp % pair
    rows, width = xv.shape
    depth, units = up_hbm.shape
    n_chunk = down_hbm.shape[1] // LANES
    u_rows = depth // UP_STAGES
    stages = UP_STAGES + n_chunk
    wide = cores * LANES
    n_v = n_chunk * n_x
    xs, ms, hops = range(1, n_x), range(1, pair), range(1, n_g)
    low_part = portion(u_rows, 1, 4), portion(units, 9, 16)

    def at_x(k):
        return {"img": lax.rem(x + k, n_x) * cores + c, "tp": tp}

    def at_m(k):
        return {"img": img, "tp": g * pair + lax.rem(m + k, pair)}

    def at_g(k):
        return {"img": img, "tp": lax.rem(g + k, n_g) * pair + m}

    partner = {"img": x * cores + (cores - 1 - c), "tp": tp}

    def is_up(s):
        return isinstance(s, int) and s < UP_STAGES

    def kind(s):
        return 0 if is_up(s) else 1

    def x_from(k):
        return lax.rem(x - k + n_x, n_x)

    def block(s, kx, km, core, part=None):
        src_x = x_from(kx)
        src_m = lax.rem(m - km + pair, pair)
        size = u_rows if is_up(s) else units
        cut = low_part[kind(s)]
        off, size = {None: (0, size), 0: (0, cut), 1: (cut, size - cut)}[part]
        if is_up(s):
            lo = (src_x * cores + core) * depth + s * u_rows + off
            return upf.at[src_m, pl.ds(pl.multiple_of(lo, 16), size), :]
        lo = src_m * units + off
        return dn.at[(s - UP_STAGES) * n_x + src_x, pl.ds(pl.multiple_of(lo, 16), size),
                     pl.ds(pl.multiple_of(core * LANES, LANES), LANES)]

    def copy(src, dst, send, recv, device):
        return pltpu.make_async_remote_copy(
            src_ref=src, dst_ref=dst, send_sem=send, recv_sem=recv,
            device_id=device, device_id_type=MESH)

    def direct_x(s, k, ref):
        return copy(ref, ref, dx_s.at[kind(s), k - 1], dx_r.at[s, k - 1], at_x(k))

    def direct_m(s, k, ref):
        return copy(ref, ref, dm_s.at[kind(s), k - 1], dm_r.at[s, k - 1], at_m(k))

    def relay_m(s, kx, km, ref):
        return copy(ref, ref, r1_s.at[kind(s), kx - 1, km - 1], r1_r.at[s, kx - 1, km - 1], at_m(km))

    def relay_x(s, kx, km, ref):
        return copy(ref, ref, r2_s.at[kind(s), kx - 1, km - 1], r2_r.at[s, kx - 1, km - 1], at_x(kx))

    def across(s, kx, km, ref):
        return copy(ref, ref, p_s.at[kind(s)], p_r.at[s, km if is_up(s) else kx], partner)

    def issue(s):
        ref = block(s, 0, 0, c)
        for k in ms:
            direct_m(s, k, ref).start()
        for k in xs:
            direct_x(s, k, ref).start()
        if cores > 1:
            across(s, 0, 0, ref).start()

    def forward(s):
        for km in ms:
            ref = block(s, 0, km, c)
            direct_m(s, km, ref).wait_recv()
            if cores > 1:
                across(s, 0, km, ref).start()
            for k in xs:
                relay_x(s, k, km, block(s, 0, km, c, 1)).start()
        for k in xs:
            ref = block(s, k, 0, c)
            direct_x(s, k, ref).wait_recv()
            for km in ms:
                relay_m(s, k, km, block(s, k, 0, c, 0)).start()
            if cores > 1:
                across(s, k, 0, ref).start()

    def collect(s, k):
        for km in ms:
            relay_m(s, k, km, block(s, k, km, c, 0)).wait_recv()
            relay_x(s, k, km, block(s, k, km, c, 1)).wait_recv()
            if cores > 1:
                across(s, k, km, block(s, k, km, c)).start()

    def take_up(s, km):
        if cores > 1:
            ref = upf.at[0, pl.ds(0, n_x * u_rows), :]
            across(s, 0, km, ref).wait_recv()

    def take(s, k):
        if cores > 1:
            ref = dn.at[(s - UP_STAGES) * n_x + x_from(k), :,
                        pl.ds(pl.multiple_of((cores - 1 - c) * LANES, LANES), LANES)]
            across(s, k, 0, ref).wait_recv()

    def own_down(j):
        return pltpu.make_async_copy(
            down_hbm.at[:, pl.ds(pl.multiple_of(j * LANES, LANES), LANES)],
            block(j + UP_STAGES, 0, 0, c), own_sem.at[j])

    def half(ref, h):
        return ref.at[pl.ds(h * (rows // 2), rows // 2), :]

    def token_up(e, h):
        src = xv if e == 0 else tok.at[g - e]
        return copy(half(src, h), half(tok.at[g - e], h), tu_s.at[e], tu_r.at[e, h], at_g(1))

    def token_down(e, h):
        src = xv if e == 0 else tok.at[g + e]
        return copy(half(src, h), half(tok.at[g + e], h), td_s.at[e], td_r.at[e, h], at_g(n_g - 1))

    def token_start(e):
        for h in range(2):
            @pl.when((g >= e) & (g < n_g - 1))
            def _():
                if e > 0:
                    ref = half(tok.at[g - e], h)
                    copy(ref, ref, tu_s.at[e], tu_r.at[e - 1, h], at_g(1)).wait_recv()
                token_up(e, h).start()

            @pl.when((g <= n_g - 1 - e) & (g > 0))
            def _():
                if e > 0:
                    ref = half(tok.at[g + e], h)
                    copy(ref, ref, td_s.at[e], td_r.at[e - 1, h], at_g(n_g - 1)).wait_recv()
                token_down(e, h).start()

    def token_end():
        for e in hops:
            for h in range(2):
                @pl.when((g >= e) & (g == n_g - 1))
                def _():
                    ref = half(tok.at[g - e], h)
                    copy(ref, ref, tu_s.at[0], tu_r.at[e - 1, h], at_g(1)).wait_recv()

                @pl.when((g <= n_g - 1 - e) & (g == 0))
                def _():
                    ref = half(tok.at[g + e], h)
                    copy(ref, ref, td_s.at[0], td_r.at[e - 1, h], at_g(n_g - 1)).wait_recv()

    def bias(k, src, slot):
        return copy(src, ubf.at[slot], bs_s.at[slot], bs_r.at[slot], at_m(k))

    def upward(v, d):
        return copy(pb.at[v, d], from_low.at[v, d], lo_s.at[d - 1], lo_r.at[v, d - 1], at_g(1))

    def downward(v, d):
        return copy(pb.at[v, d], from_high.at[v, d], hi_s.at[d], hi_r.at[v, d], at_g(n_g - 1))

    def normalize(values, at):
        values = values.astype(jnp.float32)
        center = jnp.mean(values, axis=1, keepdims=True)
        spread = jnp.mean((values - center) ** 2, axis=1, keepdims=True)
        lines = (values - center) * lax.rsqrt(spread + 1e-05) * gain[...] + nbias[...]
        normed[pl.ds(pl.multiple_of(at * rows, rows), rows), :] = lines.astype(jnp.bfloat16)

    barrier = pltpu.get_barrier_semaphore()
    near = [at_x(k) for k in xs] + [at_m(k) for k in ms]
    if cores > 1:
        near.append(partner)

    def greet(device):
        pl.semaphore_signal(barrier, inc=1, device_id=device, device_id_type=MESH)

    for device in near:
        greet(device)

    @pl.when(g < n_g - 1)
    def _():
        greet(at_g(1))

    @pl.when(g > 0)
    def _():
        greet(at_g(n_g - 1))

    own_up = upf.at[m, pl.ds(pl.multiple_of(img * depth, depth), depth), :]
    loads = [pltpu.make_async_copy(a, b, in_sem.at[i]) for i, (a, b) in enumerate((
        (x_hbm, xv), (up_hbm, own_up), (gain_hbm, gain), (nbias_hbm, nbias), (ubias_hbm, ubias), (dbias_hbm, dbias)))]
    for load in loads:
        load.start()
    for j in range(n_chunk):
        own_down(j).start()
    for i in (0, 2, 3, 4, 1):
        loads[i].wait()
    normalize(xv[...], g)

    ends = (g + n_g - 1) // n_g + (2 * n_g - 2 - g) // n_g
    pl.semaphore_wait(barrier, len(near) + ends)

    for s in range(UP_STAGES):
        issue(s)
    if n_g > 1:
        token_start(0)
    for k in ms:
        bias(k, ubias, k - 1).start()
    loads[5].wait()

    def up_rows(km):
        place = lax.rem(m - km + pair, pair)
        biases = ubias if km == 0 else ubf.at[km - 1]

        def up_tile(n, carry):
            cols = pl.ds(pl.multiple_of(n * TILE, TILE), TILE)
            summed = jnp.dot(normed[...], upf[place, :, cols], preferred_element_type=jnp.float32)
            at = pl.ds(pl.multiple_of(place * units + n * TILE, TILE), TILE)
            hidden[:, at] = jax.nn.gelu(summed + biases[:, cols]).astype(jnp.bfloat16)
            return carry

        lax.fori_loop(0, units // TILE, up_tile, 0)

    for s in range(max(UP_STAGES, n_g - 1)):
        if 0 < s + 1 < n_g - 1:
            token_start(s + 1)
        if s < UP_STAGES:
            forward(s)
    for j in range(min(2, n_chunk)):
        own_down(j).wait()
        issue(UP_STAGES + j)
    token_end()
    for k in hops:
        o = lax.rem(g + k, n_g)
        normalize(tok[o], o)
    for s in range(UP_STAGES):
        take_up(s, 0)
    up_rows(0)
    for s in range(UP_STAGES):
        for k in xs:
            collect(s, k)
    for km in ms:
        bias(km, ubias, km - 1).wait_recv()
        for s in range(UP_STAGES):
            take_up(s, km)
        up_rows(km)

    def multiply(v, j, k):
        value = jnp.dot(hidden[...], dn[j * n_x + x_from(k)], preferred_element_type=jnp.float32)
        pb[v] = value.reshape(n_g, rows, wide).astype(jnp.bfloat16)

    def pass_on(step):
        v_up, v_down = step - LAG * g, step - LAG * (n_g - 1 - g)
        go_up = (g < n_g - 1) & (v_up >= 0) & (v_up < n_v)
        go_down = (g > 0) & (v_down >= 0) & (v_down < n_v)

        def accumulate(v, d, copies, arrived):
            copies(v, d).wait_recv()
            pb[v, d] = (pb[v, d].astype(jnp.float32) + arrived[v, d].astype(jnp.float32)).astype(jnp.bfloat16)

        for k in range(n_g - 1):
            high, low = n_g - 1 - k, k

            @pl.when(go_up & (g > 0) & (g < high))
            def _():
                accumulate(v_up, high, upward, from_low)

            @pl.when(go_down & (g < n_g - 1) & (g > low))
            def _():
                accumulate(v_down, low, downward, from_high)

            @pl.when(go_up & (g < high))
            def _():
                upward(v_up, high).start()

            @pl.when(go_down & (g > low))
            def _():
                downward(v_down, low).start()

    def out_copy(cols):
        return pltpu.make_async_copy(ov.at[:, cols], out_hbm.at[:, cols], out_sem.at[0])

    def reduce(v):
        some = (v + n_v - 1) // n_v
        i = (v + n_x - 1) // n_x
        k = lax.rem(v + n_x - 1, n_x) * some + i // n_chunk
        j = i - (k + n_x - 1) // n_x

        @pl.when(g > 0)
        def _():
            upward(v, g).wait_recv()

        @pl.when(g < n_g - 1)
        def _():
            downward(v, g).wait_recv()

        src_x = x_from(k)
        for core in range(cores):
            cols = pl.ds(pl.multiple_of(((src_x * cores + core) * n_chunk + j) * LANES, LANES), LANES)
            piece = slice(core * LANES, (core + 1) * LANES)
            total = pb[v, g, :, piece].astype(jnp.float32) + dbias[:, cols]
            below = from_low[v, g, :, piece].astype(jnp.float32)
            above = from_high[v, g, :, piece].astype(jnp.float32)
            total = total + jnp.where(g > 0, below, 0.0) + jnp.where(g < n_g - 1, above, 0.0)
            ov[:, cols] = total.astype(jnp.bfloat16)
            out_copy(cols).start()

    settle = LAG * (n_g - 1) + 1

    def unit(v, j, k):
        take(j + UP_STAGES, k)
        multiply(v, j, k)
        pass_on(v)

        @pl.when(v >= settle)
        def _():
            reduce(v - settle)

    def later(i, base, first):
        def one(k, carry):
            collect(i + UP_STAGES, k)
            unit(base + k, i, k)
            return carry

        lax.fori_loop(1, n_x, one, 0)

    def tick(i, carry):
        forward(i + UP_STAGES)

        @pl.when(i + 2 < n_chunk)
        def _():
            own_down(i + 2).wait()
            issue(i + 2 + UP_STAGES)

        unit(n_x * (i - 1) + 1, i, 0)
        later(i - 1, n_x * (i - 1) + 1, True)
        return carry

    forward(UP_STAGES)
    if n_chunk > 2:
        own_down(2).wait()
        issue(2 + UP_STAGES)
    unit(0, 0, 0)
    lax.fori_loop(1, n_chunk, tick, 0)
    later(n_chunk - 1, n_x * (n_chunk - 1), False)

    def drain(step, carry):
        pass_on(step)
        return carry

    def reduce_tick(v, carry):
        reduce(v)
        return carry

    lax.fori_loop(n_v, n_v + LAG * (n_g - 2), drain, 0)
    lax.fori_loop(max(n_v - settle, 0), n_v, reduce_tick, 0)

    for t in range(2):
        s = 0 if t == 0 else UP_STAGES
        cut = low_part[t]

        def span(size):
            if t == 0:
                return upf.at[0, pl.ds(0, UP_STAGES * size), :]
            return dn.at[pl.ds(0, n_chunk), pl.ds(0, size), pl.ds(0, LANES)]

        full = u_rows if t == 0 else units
        for k in xs:
            direct_x(s, k, span(full)).wait_send()
        for k in ms:
            direct_m(s, k, span(full)).wait_send()
        for k in xs:
            for km in ms:
                relay_m(s, k, km, span(cut)).wait_send()
                relay_x(s, k, km, span(full - cut)).wait_send()
        if cores > 1:
            ref = upf.at[:, pl.ds(0, n_x * depth), :] if t == 0 else dn.at[:, :, pl.ds(0, LANES)]
            across(s, 0, 0, ref).wait_send()
    for d in range(n_g):
        @pl.when(g < d)
        def _():
            ref = pb.at[:, d]
            copy(ref, ref, lo_s.at[d - 1], lo_r.at[0, 0], at_g(1)).wait_send()

        @pl.when(g > d)
        def _():
            ref = pb.at[:, d]
            copy(ref, ref, hi_s.at[d], hi_r.at[0, 0], at_g(n_g - 1)).wait_send()
    for e in range(n_g - 1):
        @pl.when((g >= e) & (g < n_g - 1))
        def _():
            copy(tok.at[0], tok.at[0], tu_s.at[e], tu_r.at[e, 0], at_g(1)).wait_send()

        @pl.when((g <= n_g - 1 - e) & (g > 0))
        def _():
            copy(tok.at[0], tok.at[0], td_s.at[e], td_r.at[e, 0], at_g(n_g - 1)).wait_send()
    for k in ms:
        bias(k, ubias, k - 1).wait_send()
    pltpu.make_async_copy(ov, out_hbm, out_sem.at[0]).wait()


def solution(mesh):
    n_img, n_tp = mesh.shape["img"], mesh.shape["tp"]
    cores = 2 if n_img % 2 == 0 else 1
    pair = 2 if n_tp % 2 == 0 else 1
    n_x, n_g = n_img // cores, n_tp // pair

    def on_device(x, gain, nbias, up, ubias, down, dbias):
        rows, width = x.shape
        depth, units = up.shape
        n_chunk = down.shape[1] // LANES
        stages = UP_STAGES + n_chunk
        n_v, wide = n_chunk * n_x, cores * LANES
        out_width = n_img * down.shape[1]
        bf16, f32 = jnp.bfloat16, jnp.float32
        dma = pltpu.SemaphoreType.DMA
        ox, om, og = max(n_x - 1, 1), max(pair - 1, 1), max(n_g - 1, 1)
        scratch = [
            pltpu.VMEM((rows, width), bf16),
            pltpu.VMEM((1, width), f32),
            pltpu.VMEM((1, width), f32),
            pltpu.VMEM((1, units), f32),
            pltpu.VMEM((1, out_width), f32),
            pltpu.VMEM((n_g, rows, width), bf16),
            pltpu.VMEM((n_g * rows, width), bf16),
            pltpu.VMEM((pair, width, units), bf16),
            pltpu.VMEM((om, 1, units), f32),
            pltpu.VMEM((n_g * rows, pair * units), bf16),
            pltpu.VMEM((n_v, pair * units, wide), bf16),
            pltpu.VMEM((n_v, n_g, rows, wide), bf16),
            pltpu.VMEM((n_v, n_g, rows, wide), bf16),
            pltpu.VMEM((n_v, n_g, rows, wide), bf16),
            pltpu.VMEM((rows, out_width), bf16),
        ]
        scratch += [dma((6,)), dma((n_chunk,)), dma((1,))]
        scratch += [dma((og,)), dma((og, 2))] * 2 + [dma((om,))] * 2
        scratch += [dma((2, ox)), dma((stages, ox)), dma((2, om)), dma((stages, om))]
        scratch += [dma((2, ox, om)), dma((stages, ox, om))] * 2
        scratch += [dma((2,)), dma((stages, max(n_x, pair)))]
        scratch += [dma((og,)), dma((n_v, og))] * 2
        return pl.pallas_call(
            functools.partial(kernel, n_img, n_tp),
            out_shape=jax.ShapeDtypeStruct((rows, out_width), bf16),
            in_specs=[pl.BlockSpec(memory_space=pl.ANY)] * 7,
            out_specs=pl.BlockSpec(memory_space=pl.ANY),
            scratch_shapes=scratch,
            compiler_params=pltpu.CompilerParams(
                collective_id=0, has_side_effects=True, vmem_limit_bytes=60 * 1024 * 1024),
        )(x, gain.reshape(1, -1), nbias.reshape(1, -1), up, ubias.reshape(1, -1), down,
          dbias.reshape(1, -1))

    return jax.shard_map(
        on_device,
        mesh=mesh,
        in_specs=(P(("img", "tp"), None), P(), P(), P("img", "tp"), P("tp"), P("tp", "img"), P()),
        out_specs=P(("img", "tp"), None),
        check_vma=False,
    )
```

```python
import functools

import jax
import jax.numpy as jnp
from jax import lax
from jax.experimental import pallas as pl
from jax.experimental.pallas import tpu as pltpu
from jax.sharding import PartitionSpec as P

MESH = pl.DeviceIdType.MESH
LANES = 128
UP_STAGES = 2
LAG = 2
TILE = 256


def portion(size, num, den):
    return max(size * num // den // 16 * 16, 16)


def kernel(n_img, n_tp, x_hbm, gain_hbm, nbias_hbm, up_hbm, ubias_hbm, down_hbm, dbias_hbm, out_ref,
           xv, gain, nbias, ubias, dbias, tok, normed, upf, ubf, hidden, dn, pb, from_low, from_high,
           in_sem, own_sem, tu_s, tu_r, td_s, td_r, bs_s, bs_r,
           dx_s, dx_r, dm_s, dm_r, r1_s, r1_r, r2_s, r2_r, p_s, p_r, lo_s, lo_r, hi_s, hi_r):
    cores = 2 if n_img % 2 == 0 else 1
    pair = 2 if n_tp % 2 == 0 else 1
    n_x, n_g = n_img // cores, n_tp // pair
    img, tp = lax.axis_index("img"), lax.axis_index("tp")
    x, c = img // cores, img % cores
    g, m = tp // pair, tp % pair
    rows, width = xv.shape
    depth, units = up_hbm.shape
    n_chunk = down_hbm.shape[1] // LANES
    u_rows = depth // UP_STAGES
    stages = UP_STAGES + n_chunk
    wide = cores * LANES
    n_v = n_chunk * n_x
    xs, ms, hops = range(1, n_x), range(1, pair), range(1, n_g)
    low_part = portion(u_rows, 3, 8), portion(units, 17, 32)

    def at_x(k):
        return {"img": lax.rem(x + k, n_x) * cores + c, "tp": tp}

    def at_m(k):
        return {"img": img, "tp": g * pair + lax.rem(m + k, pair)}

    def at_g(k):
        return {"img": img, "tp": lax.rem(g + k, n_g) * pair + m}

    partner = {"img": x * cores + (cores - 1 - c), "tp": tp}

    def is_up(s):
        return isinstance(s, int) and s < UP_STAGES

    def kind(s):
        return 0 if is_up(s) else 1

    def x_from(k):
        return lax.rem(x - k + n_x, n_x)

    def block(s, kx, km, core, part=None):
        src_x = x_from(kx)
        src_m = lax.rem(m - km + pair, pair)
        size = u_rows if is_up(s) else units
        cut = low_part[kind(s)]
        off, size = {None: (0, size), 0: (0, cut), 1: (cut, size - cut)}[part]
        if is_up(s):
            lo = (src_x * cores + core) * depth + s * u_rows + off
            return upf.at[src_m, pl.ds(pl.multiple_of(lo, 16), size), :]
        lo = src_m * units + off
        return dn.at[(s - UP_STAGES) * n_x + src_x, pl.ds(pl.multiple_of(lo, 16), size),
                     pl.ds(pl.multiple_of(core * LANES, LANES), LANES)]

    def copy(src, dst, send, recv, device):
        return pltpu.make_async_remote_copy(
            src_ref=src, dst_ref=dst, send_sem=send, recv_sem=recv,
            device_id=device, device_id_type=MESH)

    def direct_x(s, k, ref):
        return copy(ref, ref, dx_s.at[kind(s), k - 1], dx_r.at[s, k - 1], at_x(k))

    def direct_m(s, k, ref):
        return copy(ref, ref, dm_s.at[kind(s), k - 1], dm_r.at[s, k - 1], at_m(k))

    def relay_m(s, kx, km, ref):
        return copy(ref, ref, r1_s.at[kind(s), kx - 1, km - 1], r1_r.at[s, kx - 1, km - 1], at_m(km))

    def relay_x(s, kx, km, ref):
        return copy(ref, ref, r2_s.at[kind(s), kx - 1, km - 1], r2_r.at[s, kx - 1, km - 1], at_x(kx))

    def across(s, kx, km, ref):
        return copy(ref, ref, p_s.at[kind(s)], p_r.at[s, km if is_up(s) else kx], partner)

    def issue(s):
        ref = block(s, 0, 0, c)
        for k in ms:
            direct_m(s, k, ref).start()
        for k in xs:
            direct_x(s, k, ref).start()
        if cores > 1:
            across(s, 0, 0, ref).start()

    def forward_m(s):
        for km in ms:
            ref = block(s, 0, km, c)
            direct_m(s, km, ref).wait_recv()
            if cores > 1:
                across(s, 0, km, ref).start()
            for k in xs:
                relay_x(s, k, km, block(s, 0, km, c, 1)).start()

    def forward_x(s):
        for k in xs:
            ref = block(s, k, 0, c)
            direct_x(s, k, ref).wait_recv()
            for km in ms:
                relay_m(s, k, km, block(s, k, 0, c, 0)).start()
            if cores > 1:
                across(s, k, 0, ref).start()

    def collect(s, k):
        for km in ms:
            relay_m(s, k, km, block(s, k, km, c, 0)).wait_recv()
            relay_x(s, k, km, block(s, k, km, c, 1)).wait_recv()
            if cores > 1:
                across(s, k, km, block(s, k, km, c)).start()

    def take_up(s, km):
        if cores > 1:
            ref = upf.at[0, pl.ds(0, n_x * u_rows), :]
            across(s, 0, km, ref).wait_recv()

    def take(s, k):
        if cores > 1:
            ref = dn.at[(s - UP_STAGES) * n_x + x_from(k), :,
                        pl.ds(pl.multiple_of((cores - 1 - c) * LANES, LANES), LANES)]
            across(s, k, 0, ref).wait_recv()

    def own_down(j):
        return pltpu.make_async_copy(
            down_hbm.at[:, pl.ds(pl.multiple_of(j * LANES, LANES), LANES)],
            block(j + UP_STAGES, 0, 0, c), own_sem.at[j])

    def half(ref, h):
        return ref.at[pl.ds(h * (rows // 2), rows // 2), :]

    def token_up(e, h):
        src = xv if e == 0 else tok.at[g - e]
        return copy(half(src, h), half(tok.at[g - e], h), tu_s.at[e], tu_r.at[e, h], at_g(1))

    def token_down(e, h):
        src = xv if e == 0 else tok.at[g + e]
        return copy(half(src, h), half(tok.at[g + e], h), td_s.at[e], td_r.at[e, h], at_g(n_g - 1))

    def token_start(e):
        for h in range(2):
            @pl.when((g >= e) & (g < n_g - 1))
            def _():
                if e > 0:
                    ref = half(tok.at[g - e], h)
                    copy(ref, ref, tu_s.at[e], tu_r.at[e - 1, h], at_g(1)).wait_recv()
                token_up(e, h).start()

            @pl.when((g <= n_g - 1 - e) & (g > 0))
            def _():
                if e > 0:
                    ref = half(tok.at[g + e], h)
                    copy(ref, ref, td_s.at[e], td_r.at[e - 1, h], at_g(n_g - 1)).wait_recv()
                token_down(e, h).start()

    def token_end():
        for e in hops:
            for h in range(2):
                @pl.when((g >= e) & (g == n_g - 1))
                def _():
                    ref = half(tok.at[g - e], h)
                    copy(ref, ref, tu_s.at[0], tu_r.at[e - 1, h], at_g(1)).wait_recv()

                @pl.when((g <= n_g - 1 - e) & (g == 0))
                def _():
                    ref = half(tok.at[g + e], h)
                    copy(ref, ref, td_s.at[0], td_r.at[e - 1, h], at_g(n_g - 1)).wait_recv()

    def bias(k, src, slot):
        return copy(src, ubf.at[slot], bs_s.at[slot], bs_r.at[slot], at_m(k))

    def upward(v, d):
        return copy(pb.at[v, d], from_low.at[v, d], lo_s.at[d - 1], lo_r.at[v, d - 1], at_g(1))

    def downward(v, d):
        return copy(pb.at[v, d], from_high.at[v, d], hi_s.at[d], hi_r.at[v, d], at_g(n_g - 1))

    def normalize(values, at):
        values = values.astype(jnp.float32)
        center = jnp.mean(values, axis=1, keepdims=True)
        spread = jnp.mean((values - center) ** 2, axis=1, keepdims=True)
        lines = (values - center) * lax.rsqrt(spread + 1e-05) * gain[...] + nbias[...]
        normed[pl.ds(pl.multiple_of(at * rows, rows), rows), :] = lines.astype(jnp.bfloat16)

    barrier = pltpu.get_barrier_semaphore()
    near = [at_x(k) for k in xs] + [at_m(k) for k in ms]
    if cores > 1:
        near.append(partner)

    def greet(device):
        pl.semaphore_signal(barrier, inc=1, device_id=device, device_id_type=MESH)

    for device in near:
        greet(device)

    @pl.when(g < n_g - 1)
    def _():
        greet(at_g(1))

    @pl.when(g > 0)
    def _():
        greet(at_g(n_g - 1))

    own_up = upf.at[m, pl.ds(pl.multiple_of(img * depth, depth), depth), :]
    loads = [pltpu.make_async_copy(a, b, in_sem.at[i]) for i, (a, b) in enumerate((
        (x_hbm, xv), (up_hbm, own_up), (gain_hbm, gain), (nbias_hbm, nbias), (ubias_hbm, ubias), (dbias_hbm, dbias)))]
    for load in loads:
        load.start()
    for j in range(n_chunk):
        own_down(j).start()
    for i in (0, 2, 3, 4, 1):
        loads[i].wait()
    normalize(xv[...], g)

    ends = (g + n_g - 1) // n_g + (2 * n_g - 2 - g) // n_g
    pl.semaphore_wait(barrier, len(near) + ends)

    for s in range(UP_STAGES):
        issue(s)
    if n_g > 1:
        token_start(0)
    for k in ms:
        bias(k, ubias, k - 1).start()
    loads[5].wait()

    def up_rows(km):
        place = lax.rem(m - km + pair, pair)
        biases = ubias if km == 0 else ubf.at[km - 1]

        def up_tile(n, carry):
            cols = pl.ds(pl.multiple_of(n * TILE, TILE), TILE)
            summed = jnp.dot(normed[...], upf[place, :, cols], preferred_element_type=jnp.float32)
            at = pl.ds(pl.multiple_of(place * units + n * TILE, TILE), TILE)
            hidden[:, at] = jax.nn.gelu(summed + biases[:, cols]).astype(jnp.bfloat16)
            return carry

        lax.fori_loop(0, units // TILE, up_tile, 0)

    for s in range(max(UP_STAGES, n_g - 1)):
        if 0 < s + 1 < n_g - 1:
            token_start(s + 1)
        if s < UP_STAGES:
            forward_m(s)
            forward_x(s)
    for j in range(min(2, n_chunk)):
        own_down(j).wait()
        issue(UP_STAGES + j)
    token_end()
    for k in hops:
        o = lax.rem(g + k, n_g)
        normalize(tok[o], o)
    for s in range(UP_STAGES):
        take_up(s, 0)
    up_rows(0)
    for s in range(UP_STAGES):
        for k in xs:
            collect(s, k)
    for km in ms:
        bias(km, ubias, km - 1).wait_recv()
        for s in range(UP_STAGES):
            take_up(s, km)
        up_rows(km)

    def multiply(v, j, k):
        value = jnp.dot(hidden[...], dn[j * n_x + x_from(k)], preferred_element_type=jnp.float32)
        pb[v] = value.reshape(n_g, rows, wide).astype(jnp.bfloat16)

    def pass_on(step):
        v_up, v_down = step - LAG * g, step - LAG * (n_g - 1 - g)
        go_up = (g < n_g - 1) & (v_up >= 0) & (v_up < n_v)
        go_down = (g > 0) & (v_down >= 0) & (v_down < n_v)

        def accumulate(v, d, copies, arrived):
            copies(v, d).wait_recv()
            pb[v, d] = (pb[v, d].astype(jnp.float32) + arrived[v, d].astype(jnp.float32)).astype(jnp.bfloat16)

        for k in range(n_g - 1):
            high, low = n_g - 1 - k, k

            @pl.when(go_up & (g > 0) & (g < high))
            def _():
                accumulate(v_up, high, upward, from_low)

            @pl.when(go_down & (g < n_g - 1) & (g > low))
            def _():
                accumulate(v_down, low, downward, from_high)

            @pl.when(go_up & (g < high))
            def _():
                upward(v_up, high).start()

            @pl.when(go_down & (g > low))
            def _():
                downward(v_down, low).start()

    def reduce(v):
        some = (v + n_v - 1) // n_v
        i = (v + n_x - 1) // n_x
        k = lax.rem(v + n_x - 1, n_x) * some + i // n_chunk
        j = i - (k + n_x - 1) // n_x

        @pl.when(g > 0)
        def _():
            upward(v, g).wait_recv()

        @pl.when(g < n_g - 1)
        def _():
            downward(v, g).wait_recv()

        src_x = x_from(k)
        for core in range(cores):
            cols = pl.ds(pl.multiple_of(((src_x * cores + core) * n_chunk + j) * LANES, LANES), LANES)
            piece = slice(core * LANES, (core + 1) * LANES)
            total = pb[v, g, :, piece].astype(jnp.float32) + dbias[:, cols]
            below = from_low[v, g, :, piece].astype(jnp.float32)
            above = from_high[v, g, :, piece].astype(jnp.float32)
            total = total + jnp.where(g > 0, below, 0.0) + jnp.where(g < n_g - 1, above, 0.0)
            out_ref[:, cols] = total.astype(jnp.bfloat16)

    settle = LAG * (n_g - 1) + 1

    def unit(v, j, k):
        take(j + UP_STAGES, k)
        multiply(v, j, k)
        pass_on(v)

        @pl.when(v >= settle)
        def _():
            reduce(v - settle)

    def later(i, base):
        def one(k, carry):
            collect(i + UP_STAGES, k)
            unit(base + k, i, k)
            return carry

        lax.fori_loop(1, n_x, one, 0)

    def start(i):
        @pl.when(i + 2 < n_chunk)
        def _():
            own_down(i + 2).wait()
            issue(i + 2 + UP_STAGES)

    def tick(i, carry):
        forward_m(i + UP_STAGES)
        unit(n_x * (i - 1) + 1, i, 0)
        forward_x(i + UP_STAGES)
        start(i)
        later(i - 1, n_x * (i - 1) + 1)
        return carry

    forward_m(UP_STAGES)
    unit(0, 0, 0)
    forward_x(UP_STAGES)
    start(0)
    lax.fori_loop(1, n_chunk, tick, 0)
    later(n_chunk - 1, n_x * (n_chunk - 1))

    def drain(step, carry):
        pass_on(step)
        return carry

    def reduce_tick(v, carry):
        reduce(v)
        return carry

    lax.fori_loop(n_v, n_v + LAG * (n_g - 2), drain, 0)
    lax.fori_loop(max(n_v - settle, 0), n_v, reduce_tick, 0)

    for t in range(2):
        s = 0 if t == 0 else UP_STAGES
        cut = low_part[t]

        def span(size):
            if t == 0:
                return upf.at[0, pl.ds(0, UP_STAGES * size), :]
            return dn.at[pl.ds(0, n_chunk), pl.ds(0, size), pl.ds(0, LANES)]

        full = u_rows if t == 0 else units
        for k in xs:
            direct_x(s, k, span(full)).wait_send()
        for k in ms:
            direct_m(s, k, span(full)).wait_send()
        for k in xs:
            for km in ms:
                relay_m(s, k, km, span(cut)).wait_send()
                relay_x(s, k, km, span(full - cut)).wait_send()
        if cores > 1:
            ref = upf.at[:, pl.ds(0, n_x * depth), :] if t == 0 else dn.at[:, :, pl.ds(0, LANES)]
            across(s, 0, 0, ref).wait_send()
    for d in range(n_g):
        @pl.when(g < d)
        def _():
            ref = pb.at[:, d]
            copy(ref, ref, lo_s.at[d - 1], lo_r.at[0, 0], at_g(1)).wait_send()

        @pl.when(g > d)
        def _():
            ref = pb.at[:, d]
            copy(ref, ref, hi_s.at[d], hi_r.at[0, 0], at_g(n_g - 1)).wait_send()
    for e in range(n_g - 1):
        @pl.when((g >= e) & (g < n_g - 1))
        def _():
            copy(tok.at[0], tok.at[0], tu_s.at[e], tu_r.at[e, 0], at_g(1)).wait_send()

        @pl.when((g <= n_g - 1 - e) & (g > 0))
        def _():
            copy(tok.at[0], tok.at[0], td_s.at[e], td_r.at[e, 0], at_g(n_g - 1)).wait_send()
    for k in ms:
        bias(k, ubias, k - 1).wait_send()


def solution(mesh):
    n_img, n_tp = mesh.shape["img"], mesh.shape["tp"]
    cores = 2 if n_img % 2 == 0 else 1
    pair = 2 if n_tp % 2 == 0 else 1
    n_x, n_g = n_img // cores, n_tp // pair

    def on_device(x, gain, nbias, up, ubias, down, dbias):
        rows, width = x.shape
        depth, units = up.shape
        n_chunk = down.shape[1] // LANES
        stages = UP_STAGES + n_chunk
        n_v, wide = n_chunk * n_x, cores * LANES
        out_width = n_img * down.shape[1]
        bf16, f32 = jnp.bfloat16, jnp.float32
        dma = pltpu.SemaphoreType.DMA
        ox, om, og = max(n_x - 1, 1), max(pair - 1, 1), max(n_g - 1, 1)
        scratch = [
            pltpu.VMEM((rows, width), bf16),
            pltpu.VMEM((1, width), f32),
            pltpu.VMEM((1, width), f32),
            pltpu.VMEM((1, units), f32),
            pltpu.VMEM((1, out_width), f32),
            pltpu.VMEM((n_g, rows, width), bf16),
            pltpu.VMEM((n_g * rows, width), bf16),
            pltpu.VMEM((pair, width, units), bf16),
            pltpu.VMEM((om, 1, units), f32),
            pltpu.VMEM((n_g * rows, pair * units), bf16),
            pltpu.VMEM((n_v, pair * units, wide), bf16),
            pltpu.VMEM((n_v, n_g, rows, wide), bf16),
            pltpu.VMEM((n_v, n_g, rows, wide), bf16),
            pltpu.VMEM((n_v, n_g, rows, wide), bf16),
        ]
        scratch += [dma((6,)), dma((n_chunk,))]
        scratch += [dma((og,)), dma((og, 2))] * 2 + [dma((om,))] * 2
        scratch += [dma((2, ox)), dma((stages, ox)), dma((2, om)), dma((stages, om))]
        scratch += [dma((2, ox, om)), dma((stages, ox, om))] * 2
        scratch += [dma((2,)), dma((stages, max(n_x, pair)))]
        scratch += [dma((og,)), dma((n_v, og))] * 2
        return pl.pallas_call(
            functools.partial(kernel, n_img, n_tp),
            out_shape=pltpu.VMEM((rows, out_width), bf16),
            in_specs=[pl.BlockSpec(memory_space=pl.ANY)] * 7,
            out_specs=pl.BlockSpec(memory_space=pltpu.VMEM),
            scratch_shapes=scratch,
            compiler_params=pltpu.CompilerParams(
                collective_id=0, has_side_effects=True, vmem_limit_bytes=60 * 1024 * 1024),
        )(x, gain.reshape(1, -1), nbias.reshape(1, -1), up, ubias.reshape(1, -1), down,
          dbias.reshape(1, -1))

    return jax.shard_map(
        on_device,
        mesh=mesh,
        in_specs=(P(("img", "tp"), None), P(), P(), P("img", "tp"), P("tp"), P("tp", "img"), P()),
        out_specs=P(("img", "tp"), None),
        check_vma=False,
    )
```

```python
import functools

import jax
import jax.numpy as jnp
from jax import lax
from jax.experimental import pallas as pl
from jax.experimental.pallas import tpu as pltpu
from jax.sharding import PartitionSpec as P

MESH = pl.DeviceIdType.MESH
LANES = 128
UP_STAGES = 2
LAG = 2
TILE = 256
TAIL = 3


def portion(size, num, den):
    return max(size * num // den // 16 * 16, 16)


def kernel(n_img, n_tp, x_hbm, gain_hbm, nbias_hbm, up_hbm, ubias_hbm, down_hbm, dbias_hbm, out_ref,
           xv, gain, nbias, ubias, dbias, tok, normed, upf, ubf, hidden, dn, pb, from_low, from_high,
           in_sem, own_sem, tu_s, tu_r, td_s, td_r, bs_s, bs_r,
           dx_s, dx_r, dm_s, dm_r, r1_s, r1_r, r2_s, r2_r, p_s, p_r, lo_s, lo_r, hi_s, hi_r, end_r):
    cores = 2 if n_img % 2 == 0 else 1
    pair = 2 if n_tp % 2 == 0 else 1
    n_x, n_g = n_img // cores, n_tp // pair
    img, tp = lax.axis_index("img"), lax.axis_index("tp")
    x, c = img // cores, img % cores
    g, m = tp // pair, tp % pair
    rows, width = xv.shape
    depth, units = up_hbm.shape
    n_chunk = down_hbm.shape[1] // LANES
    u_rows = depth // UP_STAGES
    stages = UP_STAGES + n_chunk
    wide = cores * LANES
    n_v = n_chunk * n_x
    v_last, v_tail = n_v - 1, n_v - TAIL
    xs, ms, hops = range(1, n_x), range(1, pair), range(1, n_g)
    n_tile = units // TILE
    low_part = portion(u_rows, 1, 4), portion(units, 9, 16)

    def at_x(k):
        return {"img": lax.rem(x + k, n_x) * cores + c, "tp": tp}

    def at_m(k):
        return {"img": img, "tp": g * pair + lax.rem(m + k, pair)}

    def at_g(k):
        return {"img": img, "tp": lax.rem(g + k, n_g) * pair + m}

    partner = {"img": x * cores + (cores - 1 - c), "tp": tp}

    def is_up(s):
        return isinstance(s, int) and s < UP_STAGES

    def kind(s):
        return 0 if is_up(s) else 1

    def x_from(k):
        return lax.rem(x - k + n_x, n_x)

    def block(s, kx, km, core, part=None):
        src_x = x_from(kx)
        src_m = lax.rem(m - km + pair, pair)
        size = u_rows if is_up(s) else units
        cut = low_part[kind(s)]
        off, size = {None: (0, size), 0: (0, cut), 1: (cut, size - cut)}[part]
        if is_up(s):
            lo = (src_x * cores + core) * depth + s * u_rows + off
            return upf.at[src_m, pl.ds(pl.multiple_of(lo, 16), size), :]
        lo = src_m * units + off
        return dn.at[(s - UP_STAGES) * n_x + src_x, pl.ds(pl.multiple_of(lo, 16), size),
                     pl.ds(pl.multiple_of(core * LANES, LANES), LANES)]

    def copy(src, dst, send, recv, device):
        return pltpu.make_async_remote_copy(
            src_ref=src, dst_ref=dst, send_sem=send, recv_sem=recv,
            device_id=device, device_id_type=MESH)

    def direct_x(s, k, ref):
        return copy(ref, ref, dx_s.at[kind(s), k - 1], dx_r.at[s, k - 1], at_x(k))

    def direct_m(s, k, ref):
        return copy(ref, ref, dm_s.at[kind(s), k - 1], dm_r.at[s, k - 1], at_m(k))

    def relay_m(s, kx, km, ref):
        return copy(ref, ref, r1_s.at[kind(s), kx - 1, km - 1], r1_r.at[s, kx - 1, km - 1], at_m(km))

    def relay_x(s, kx, km, ref):
        return copy(ref, ref, r2_s.at[kind(s), kx - 1, km - 1], r2_r.at[s, kx - 1, km - 1], at_x(kx))

    def across(s, kx, km, ref):
        return copy(ref, ref, p_s.at[kind(s)], p_r.at[s, km if is_up(s) else kx], partner)

    def issue_m(s):
        ref = block(s, 0, 0, c)
        for k in ms:
            direct_m(s, k, ref).start()
        if cores > 1:
            across(s, 0, 0, ref).start()

    def issue_x(s):
        ref = block(s, 0, 0, c)
        for k in xs:
            direct_x(s, k, ref).start()

    def issue(s):
        issue_m(s)
        issue_x(s)

    def forward_m(s):
        for km in ms:
            ref = block(s, 0, km, c)
            direct_m(s, km, ref).wait_recv()
            if cores > 1:
                across(s, 0, km, ref).start()
            for k in xs:
                relay_x(s, k, km, block(s, 0, km, c, 1)).start()

    def forward_x(s):
        for k in xs:
            ref = block(s, k, 0, c)
            direct_x(s, k, ref).wait_recv()
            for km in ms:
                relay_m(s, k, km, block(s, k, 0, c, 0)).start()
            if cores > 1:
                across(s, k, 0, ref).start()

    def collect(s, k):
        for km in ms:
            for part, relay in enumerate((relay_m, relay_x)):
                ref = block(s, k, km, c, part)
                relay(s, k, km, ref).wait_recv()
                if cores > 1:
                    across(s, k, km, ref).start()

    def take_up(s, km):
        if cores > 1:
            ref = upf.at[0, pl.ds(0, n_x * u_rows), :]
            across(s, 0, km, ref).wait_recv()

    def take(s, k):
        if cores > 1:
            ref = dn.at[(s - UP_STAGES) * n_x + x_from(k), :,
                        pl.ds(pl.multiple_of((cores - 1 - c) * LANES, LANES), LANES)]
            across(s, k, 0, ref).wait_recv()

    def own_down(j):
        return pltpu.make_async_copy(
            down_hbm.at[:, pl.ds(pl.multiple_of(j * LANES, LANES), LANES)],
            block(j + UP_STAGES, 0, 0, c), own_sem.at[j])

    def half(ref, h):
        return ref.at[pl.ds(h * (rows // 2), rows // 2), :]

    def token_up(e, h):
        src = xv if e == 0 else tok.at[g - e]
        return copy(half(src, h), half(tok.at[g - e], h), tu_s.at[e], tu_r.at[e, h], at_g(1))

    def token_down(e, h):
        src = xv if e == 0 else tok.at[g + e]
        return copy(half(src, h), half(tok.at[g + e], h), td_s.at[e], td_r.at[e, h], at_g(n_g - 1))

    def token_start(e):
        for h in range(2):
            @pl.when((g >= e) & (g < n_g - 1))
            def _():
                if e > 0:
                    ref = half(tok.at[g - e], h)
                    copy(ref, ref, tu_s.at[e], tu_r.at[e - 1, h], at_g(1)).wait_recv()
                token_up(e, h).start()

            @pl.when((g <= n_g - 1 - e) & (g > 0))
            def _():
                if e > 0:
                    ref = half(tok.at[g + e], h)
                    copy(ref, ref, td_s.at[e], td_r.at[e - 1, h], at_g(n_g - 1)).wait_recv()
                token_down(e, h).start()

    def token_end():
        for e in hops:
            for h in range(2):
                @pl.when((g >= e) & (g == n_g - 1))
                def _():
                    ref = half(tok.at[g - e], h)
                    copy(ref, ref, tu_s.at[0], tu_r.at[e - 1, h], at_g(1)).wait_recv()

                @pl.when((g <= n_g - 1 - e) & (g == 0))
                def _():
                    ref = half(tok.at[g + e], h)
                    copy(ref, ref, td_s.at[0], td_r.at[e - 1, h], at_g(n_g - 1)).wait_recv()

    def bias(k, src, slot):
        return copy(src, ubf.at[slot], bs_s.at[slot], bs_r.at[slot], at_m(k))

    def upward(v, e):
        part = pl.ds(e + 1, n_g - 1 - e)
        return copy(pb.at[v, part], from_low.at[v, part], lo_s.at[0], lo_r.at[v], at_g(1))

    def downward(v, e):
        part = pl.ds(0, n_g - 1 - e)
        return copy(pb.at[v, part], from_high.at[v, part], hi_s.at[0], hi_r.at[v], at_g(n_g - 1))

    def piece_up(v, d):
        return copy(pb.at[v, d], from_low.at[v, d], lo_s.at[0], end_r.at[0, v - v_tail, d], at_g(1))

    def piece_down(v, d):
        return copy(pb.at[v, d], from_high.at[v, d], hi_s.at[0], end_r.at[1, v - v_tail, d], at_g(n_g - 1))

    def normalize(values, at):
        values = values.astype(jnp.float32)
        center = jnp.mean(values, axis=1, keepdims=True)
        spread = jnp.mean((values - center) ** 2, axis=1, keepdims=True)
        lines = (values - center) * lax.rsqrt(spread + 1e-05) * gain[...] + nbias[...]
        normed[pl.ds(pl.multiple_of(at * rows, rows), rows), :] = lines.astype(jnp.bfloat16)

    barrier = pltpu.get_barrier_semaphore()
    near = [at_x(k) for k in xs] + [at_m(k) for k in ms]
    if cores > 1:
        near.append(partner)

    def greet(device):
        pl.semaphore_signal(barrier, inc=1, device_id=device, device_id_type=MESH)

    for device in near:
        greet(device)

    @pl.when(g < n_g - 1)
    def _():
        greet(at_g(1))

    @pl.when(g > 0)
    def _():
        greet(at_g(n_g - 1))

    own_up = upf.at[m, pl.ds(pl.multiple_of(img * depth, depth), depth), :]
    loads = [pltpu.make_async_copy(a, b, in_sem.at[i]) for i, (a, b) in enumerate((
        (x_hbm, xv), (up_hbm, own_up), (gain_hbm, gain), (nbias_hbm, nbias), (ubias_hbm, ubias), (dbias_hbm, dbias)))]
    for load in loads:
        load.start()
    for j in range(n_chunk):
        own_down(j).start()
    for i in (0, 2, 3, 4, 1):
        loads[i].wait()
    normalize(xv[...], g)

    ends = (g + n_g - 1) // n_g + (2 * n_g - 2 - g) // n_g
    pl.semaphore_wait(barrier, len(near) + ends)

    for s in range(UP_STAGES):
        issue(s)
    if n_g > 1:
        token_start(0)
    for k in ms:
        bias(k, ubias, k - 1).start()
    loads[5].wait()

    def up_rows(km, first, last):
        place = lax.rem(m - km + pair, pair)
        biases = ubias if km == 0 else ubf.at[km - 1]

        def up_tile(n, carry):
            cols = pl.ds(pl.multiple_of(n * TILE, TILE), TILE)
            summed = jnp.dot(normed[...], upf[place, :, cols], preferred_element_type=jnp.float32)
            at = pl.ds(pl.multiple_of(place * units + n * TILE, TILE), TILE)
            hidden[:, at] = jax.nn.gelu(summed + biases[:, cols]).astype(jnp.bfloat16)
            return carry

        lax.fori_loop(first, last, up_tile, 0)

    for s in range(max(UP_STAGES, n_g - 1)):
        if 0 < s + 1 < n_g - 1:
            token_start(s + 1)
        if s < UP_STAGES:
            forward_m(s)
            forward_x(s)
    own_down(0).wait()
    issue(UP_STAGES)
    if n_chunk > 1:
        own_down(1).wait()
        issue_m(UP_STAGES + 1)
    token_end()
    for k in hops:
        o = lax.rem(g + k, n_g)
        normalize(tok[o], o)
    for s in range(UP_STAGES):
        take_up(s, 0)
    up_rows(0, 0, n_tile)
    for s in range(UP_STAGES):
        for k in xs:
            collect(s, k)
    for km in ms:
        bias(km, ubias, km - 1).wait_recv()
        for s in range(UP_STAGES):
            take_up(s, km)
        up_rows(km, 0, n_tile // 2)
        if km == pair - 1:
            forward_m(UP_STAGES)
            if n_chunk > 1:
                issue_x(UP_STAGES + 1)
        up_rows(km, n_tile // 2, n_tile)
    if pair == 1 and n_chunk > 1:
        issue_x(UP_STAGES + 1)

    def multiply(v, j, k):
        value = jnp.dot(hidden[...], dn[j * n_x + x_from(k)], preferred_element_type=jnp.float32)
        pb[v] = value.reshape(n_g, rows, wide).astype(jnp.bfloat16)

    upper = 2 * g // n_g
    far_d = (1 - upper) * (n_g - 1)

    def multiply_far(v, j, k):
        lines = hidden[pl.ds(pl.multiple_of(far_d * rows, rows), rows), :]
        value = jnp.dot(lines, dn[j * n_x + x_from(k)], preferred_element_type=jnp.float32)
        pb[v, far_d] = value.astype(jnp.bfloat16)

    def multiply_rest(v, j, k):
        if n_g > 1:
            lines = hidden[pl.ds(pl.multiple_of(upper * rows, rows), (n_g - 1) * rows), :]
            value = jnp.dot(lines, dn[j * n_x + x_from(k)], preferred_element_type=jnp.float32)
            pb[v, pl.ds(upper, n_g - 1)] = value.reshape(n_g - 1, rows, wide).astype(jnp.bfloat16)

    def add(v, part, arrived):
        pb[v, part] = (pb[v, part].astype(jnp.float32) + arrived[v, part].astype(jnp.float32)).astype(jnp.bfloat16)

    def pass_on(step):
        for e in reversed(range(n_g - 1)):
            v = step - LAG * e

            @pl.when((g == e) & (v >= 0) & (v < v_tail))
            def _():
                if e > 0:
                    upward(v, e - 1).wait_recv()
                    add(v, pl.ds(e + 1, n_g - 1 - e), from_low)
                upward(v, e).start()

            @pl.when((g == n_g - 1 - e) & (v >= 0) & (v < v_tail))
            def _():
                if e > 0:
                    downward(v, e - 1).wait_recv()
                    add(v, pl.ds(0, n_g - 1 - e), from_high)
                downward(v, e).start()

    def pass_pieces(step, first, stop):
        for e in reversed(range(n_g - 1)):
            v = step - LAG * e
            for i in range(first, min(stop, n_g - 1 - e)):
                for here, d, piece, arrived in (
                        (e, n_g - 1 - i, piece_up, from_low), (n_g - 1 - e, i, piece_down, from_high)):
                    @pl.when((g == here) & (v >= v_tail) & (v < n_v))
                    def _():
                        if e > 0:
                            piece(v, d).wait_recv()
                            add(v, d, arrived)
                        piece(v, d).start()

    def pass_far(step):
        pass_on(step)
        pass_pieces(step, 0, 1)

    def pass_near(step):
        pass_pieces(step, 1, n_g)

    def reduce(v):
        some = (v + n_v - 1) // n_v
        i = (v + n_x - 1) // n_x
        k = lax.rem(v + n_x - 1, n_x) * some + i // n_chunk
        j = i - (k + n_x - 1) // n_x
        for d in range(n_g):
            @pl.when(g == d)
            def _():
                if isinstance(v, int) and v >= v_tail:
                    if d > 0:
                        piece_up(v, d).wait_recv()
                    if d < n_g - 1:
                        piece_down(v, d).wait_recv()
                elif n_g > 1:
                    if d == n_g - 1:
                        upward(v, d - 1).wait_recv()
                    if d == 0:
                        downward(v, n_g - 2).wait_recv()

        src_x = x_from(k)
        for core in range(cores):
            cols = pl.ds(pl.multiple_of(((src_x * cores + core) * n_chunk + j) * LANES, LANES), LANES)
            piece = slice(core * LANES, (core + 1) * LANES)
            total = pb[v, g, :, piece].astype(jnp.float32) + dbias[:, cols]
            below = from_low[v, g, :, piece].astype(jnp.float32)
            above = from_high[v, g, :, piece].astype(jnp.float32)
            total = total + jnp.where(g > 0, below, 0.0) + jnp.where(g < n_g - 1, above, 0.0)
            out_ref[:, cols] = total.astype(jnp.bfloat16)

    settle = LAG * (n_g - 1) + 1

    def settled(v):
        @pl.when(v >= settle)
        def _():
            reduce(v - settle)

    def unit(v, j, k):
        take(j + UP_STAGES, k)
        multiply(v, j, k)
        pass_far(v)

        @pl.when(v < n_v - 2)
        def _():
            pass_near(v)

        settled(v)

    def last_unit(j, k):
        take(j + UP_STAGES, k)
        multiply_far(v_last, j, k)
        pass_far(v_last)
        multiply_rest(v_last, j, k)
        settled(v_last)

    def later(i, base, stop):
        def one(k, carry):
            collect(i + UP_STAGES, k)
            unit(base + k, i, k)
            return carry

        lax.fori_loop(1, stop, one, 0)

    def start(i):
        @pl.when(i + 2 < n_chunk)
        def _():
            own_down(i + 2).wait()
            issue(i + 2 + UP_STAGES)

    def tick(i, carry):
        forward_m(i + UP_STAGES)
        unit(n_x * (i - 1) + 1, i, 0)
        forward_x(i + UP_STAGES)
        start(i)
        later(i - 1, n_x * (i - 1) + 1, n_x)
        return carry

    unit(0, 0, 0)
    forward_x(UP_STAGES)
    start(0)
    if n_x > 1 and n_chunk > 1:
        forward_m(1 + UP_STAGES)
        unit(1, 1, 0)
        for k in xs:
            collect(UP_STAGES, k)
        forward_x(1 + UP_STAGES)
        start(1)
        for k in xs:
            unit(1 + k, 0, k)
        lax.fori_loop(2, n_chunk, tick, 0)
        later(n_chunk - 1, n_x * (n_chunk - 1), n_x - 1)
        collect(n_chunk - 1 + UP_STAGES, n_x - 1)
        last_unit(n_chunk - 1, n_x - 1)
    else:
        lax.fori_loop(1, n_chunk - 1, tick, 0)
        forward_m(n_chunk - 1 + UP_STAGES)
        forward_x(n_chunk - 1 + UP_STAGES)
        last_unit(n_chunk - 1, 0)

    def drain(step, carry):
        pass_far(step)
        pass_near(step - 2)
        return carry

    def reduce_tick(v, carry):
        reduce(v)
        return carry

    lax.fori_loop(n_v, n_v + LAG * (n_g - 2) + 2, drain, 0)
    lax.fori_loop(max(n_v - settle, 0), v_tail, reduce_tick, 0)
    for v in range(v_tail, n_v):
        reduce(v)

    for t in range(2):
        s = 0 if t == 0 else UP_STAGES
        cut = low_part[t]

        def span(size):
            if t == 0:
                return upf.at[0, pl.ds(0, UP_STAGES * size), :]
            return dn.at[pl.ds(0, n_chunk), pl.ds(0, size), pl.ds(0, LANES)]

        full = u_rows if t == 0 else units
        for k in xs:
            direct_x(s, k, span(full)).wait_send()
        for k in ms:
            direct_m(s, k, span(full)).wait_send()
        for k in xs:
            for km in ms:
                relay_m(s, k, km, span(cut)).wait_send()
                relay_x(s, k, km, span(full - cut)).wait_send()
        if cores > 1:
            ref = upf.at[:, pl.ds(0, n_x * depth), :] if t == 0 else dn.at[:, :, pl.ds(0, LANES)]
            across(s, 0, 0, ref).wait_send()
    for e in range(n_g - 1):
        @pl.when(g == e)
        def _():
            ref = pb.at[:, pl.ds(e + 1, n_g - 1 - e)]
            copy(ref, ref, lo_s.at[0], lo_r.at[0], at_g(1)).wait_send()

        @pl.when(g == n_g - 1 - e)
        def _():
            ref = pb.at[:, pl.ds(0, n_g - 1 - e)]
            copy(ref, ref, hi_s.at[0], hi_r.at[0], at_g(n_g - 1)).wait_send()
    for e in range(n_g - 1):
        @pl.when((g >= e) & (g < n_g - 1))
        def _():
            copy(tok.at[0], tok.at[0], tu_s.at[e], tu_r.at[e, 0], at_g(1)).wait_send()

        @pl.when((g <= n_g - 1 - e) & (g > 0))
        def _():
            copy(tok.at[0], tok.at[0], td_s.at[e], td_r.at[e, 0], at_g(n_g - 1)).wait_send()
    for k in ms:
        bias(k, ubias, k - 1).wait_send()


def solution(mesh):
    n_img, n_tp = mesh.shape["img"], mesh.shape["tp"]
    cores = 2 if n_img % 2 == 0 else 1
    pair = 2 if n_tp % 2 == 0 else 1
    n_x, n_g = n_img // cores, n_tp // pair

    def on_device(x, gain, nbias, up, ubias, down, dbias):
        rows, width = x.shape
        depth, units = up.shape
        n_chunk = down.shape[1] // LANES
        stages = UP_STAGES + n_chunk
        n_v, wide = n_chunk * n_x, cores * LANES
        out_width = n_img * down.shape[1]
        bf16, f32 = jnp.bfloat16, jnp.float32
        dma = pltpu.SemaphoreType.DMA
        ox, om, og = max(n_x - 1, 1), max(pair - 1, 1), max(n_g - 1, 1)
        scratch = [
            pltpu.VMEM((rows, width), bf16),
            pltpu.VMEM((1, width), f32),
            pltpu.VMEM((1, width), f32),
            pltpu.VMEM((1, units), f32),
            pltpu.VMEM((1, out_width), f32),
            pltpu.VMEM((n_g, rows, width), bf16),
            pltpu.VMEM((n_g * rows, width), bf16),
            pltpu.VMEM((pair, width, units), bf16),
            pltpu.VMEM((om, 1, units), f32),
            pltpu.VMEM((n_g * rows, pair * units), bf16),
            pltpu.VMEM((n_v, pair * units, wide), bf16),
            pltpu.VMEM((n_v, n_g, rows, wide), bf16),
            pltpu.VMEM((n_v, n_g, rows, wide), bf16),
            pltpu.VMEM((n_v, n_g, rows, wide), bf16),
        ]
        scratch += [dma((6,)), dma((n_chunk,))]
        scratch += [dma((og,)), dma((og, 2))] * 2 + [dma((om,))] * 2
        scratch += [dma((2, ox)), dma((stages, ox)), dma((2, om)), dma((stages, om))]
        scratch += [dma((2, ox, om)), dma((stages, ox, om))] * 2
        scratch += [dma((2,)), dma((stages, max(n_x, pair)))]
        scratch += [dma((1,)), dma((n_v,))] * 2 + [dma((2, TAIL, n_g))]
        return pl.pallas_call(
            functools.partial(kernel, n_img, n_tp),
            out_shape=pltpu.VMEM((rows, out_width), bf16),
            in_specs=[pl.BlockSpec(memory_space=pl.ANY)] * 7,
            out_specs=pl.BlockSpec(memory_space=pltpu.VMEM),
            scratch_shapes=scratch,
            compiler_params=pltpu.CompilerParams(
                collective_id=0, has_side_effects=True, vmem_limit_bytes=60 * 1024 * 1024),
        )(x, gain.reshape(1, -1), nbias.reshape(1, -1), up, ubias.reshape(1, -1), down,
          dbias.reshape(1, -1))

    return jax.shard_map(
        on_device,
        mesh=mesh,
        in_specs=(P(("img", "tp"), None), P(), P(), P("img", "tp"), P("tp"), P("tp", "img"), P()),
        out_specs=P(("img", "tp"), None),
        check_vma=False,
    )
```

```python
import functools

import jax
import jax.numpy as jnp
from jax import lax
from jax.experimental import pallas as pl
from jax.experimental.pallas import tpu as pltpu
from jax.sharding import PartitionSpec as P

MESH = pl.DeviceIdType.MESH
LANES = 128
UP_STAGES = 2
LAG = 2
TILE = 256
TAIL = 2


def portion(size, num, den):
    return max(size * num // den // 16 * 16, 16)


def kernel(n_img, n_tp, x_hbm, gain_hbm, nbias_hbm, up_hbm, ubias_hbm, down_hbm, dbias_hbm, out_ref,
           xv, gain, nbias, ubias, dbias, tok, normed, upf, ubf, hidden, dn, pb, from_low, from_high,
           in_sem, own_sem, tu_s, tu_r, td_s, td_r, bs_s, bs_r,
           dx_s, dx_r, dm_s, dm_r, r1_s, r1_r, r2_s, r2_r, p_s, p_r, lo_s, lo_r, hi_s, hi_r, end_r):
    cores = 2 if n_img % 2 == 0 else 1
    pair = 2 if n_tp % 2 == 0 else 1
    n_x, n_g = n_img // cores, n_tp // pair
    img, tp = lax.axis_index("img"), lax.axis_index("tp")
    x, c = img // cores, img % cores
    g, m = tp // pair, tp % pair
    rows, width = xv.shape
    depth, units = up_hbm.shape
    n_chunk = down_hbm.shape[1] // LANES
    u_rows = depth // UP_STAGES
    stages = UP_STAGES + n_chunk
    wide = cores * LANES
    n_v = n_chunk * n_x
    v_last, v_tail = n_v - 1, n_v - TAIL
    xs, ms, hops = range(1, n_x), range(1, pair), range(1, n_g)
    n_tile = units // TILE
    low_part = portion(u_rows, 1, 4), portion(units, 9, 16)

    def at_x(k):
        return {"img": lax.rem(x + k, n_x) * cores + c, "tp": tp}

    def at_m(k):
        return {"img": img, "tp": g * pair + lax.rem(m + k, pair)}

    def at_g(k):
        return {"img": img, "tp": lax.rem(g + k, n_g) * pair + m}

    partner = {"img": x * cores + (cores - 1 - c), "tp": tp}

    def is_up(s):
        return isinstance(s, int) and s < UP_STAGES

    def kind(s):
        return 0 if is_up(s) else 1

    def x_from(k):
        return lax.rem(x - k + n_x, n_x)

    def block(s, kx, km, core, part=None):
        src_x = x_from(kx)
        src_m = lax.rem(m - km + pair, pair)
        size = u_rows if is_up(s) else units
        cut = low_part[kind(s)]
        off, size = {None: (0, size), 0: (0, cut), 1: (cut, size - cut)}[part]
        if is_up(s):
            lo = (src_x * cores + core) * depth + s * u_rows + off
            return upf.at[src_m, pl.ds(pl.multiple_of(lo, 16), size), :]
        lo = src_m * units + off
        return dn.at[(s - UP_STAGES) * n_x + src_x, pl.ds(pl.multiple_of(lo, 16), size),
                     pl.ds(pl.multiple_of(core * LANES, LANES), LANES)]

    def copy(src, dst, send, recv, device):
        return pltpu.make_async_remote_copy(
            src_ref=src, dst_ref=dst, send_sem=send, recv_sem=recv,
            device_id=device, device_id_type=MESH)

    def direct_x(s, k, ref):
        return copy(ref, ref, dx_s.at[kind(s), k - 1], dx_r.at[s, k - 1], at_x(k))

    def direct_m(s, k, ref):
        return copy(ref, ref, dm_s.at[kind(s), k - 1], dm_r.at[s, k - 1], at_m(k))

    def relay_m(s, kx, km, ref):
        return copy(ref, ref, r1_s.at[kind(s), kx - 1, km - 1], r1_r.at[s, kx - 1, km - 1], at_m(km))

    def relay_x(s, kx, km, ref):
        return copy(ref, ref, r2_s.at[kind(s), kx - 1, km - 1], r2_r.at[s, kx - 1, km - 1], at_x(kx))

    def across(s, kx, km, ref):
        return copy(ref, ref, p_s.at[kind(s)], p_r.at[s, km if is_up(s) else kx], partner)

    def issue_m(s):
        ref = block(s, 0, 0, c)
        for k in ms:
            direct_m(s, k, ref).start()
        if cores > 1:
            across(s, 0, 0, ref).start()

    def issue_x(s):
        ref = block(s, 0, 0, c)
        for k in xs:
            direct_x(s, k, ref).start()

    def issue(s):
        issue_m(s)
        issue_x(s)

    def forward_m(s):
        for km in ms:
            ref = block(s, 0, km, c)
            direct_m(s, km, ref).wait_recv()
            if cores > 1:
                across(s, 0, km, ref).start()
            for k in xs:
                relay_x(s, k, km, block(s, 0, km, c, 1)).start()

    def forward_x(s):
        for k in xs:
            ref = block(s, k, 0, c)
            direct_x(s, k, ref).wait_recv()
            for km in ms:
                relay_m(s, k, km, block(s, k, 0, c, 0)).start()
            if cores > 1:
                across(s, k, 0, ref).start()

    def collect(s, k):
        for km in ms:
            for part, relay in enumerate((relay_m, relay_x)):
                ref = block(s, k, km, c, part)
                relay(s, k, km, ref).wait_recv()
                if cores > 1:
                    across(s, k, km, ref).start()

    def take_up(s, km):
        if cores > 1:
            ref = upf.at[0, pl.ds(0, n_x * u_rows), :]
            across(s, 0, km, ref).wait_recv()

    def take(s, k):
        if cores > 1:
            ref = dn.at[(s - UP_STAGES) * n_x + x_from(k), :,
                        pl.ds(pl.multiple_of((cores - 1 - c) * LANES, LANES), LANES)]
            across(s, k, 0, ref).wait_recv()

    def own_down(j):
        return pltpu.make_async_copy(
            down_hbm.at[:, pl.ds(pl.multiple_of(j * LANES, LANES), LANES)],
            block(j + UP_STAGES, 0, 0, c), own_sem.at[j])

    def half(ref, h):
        return ref.at[pl.ds(h * (rows // 2), rows // 2), :]

    def token_up(e, h):
        src = xv if e == 0 else tok.at[g - e]
        return copy(half(src, h), half(tok.at[g - e], h), tu_s.at[e], tu_r.at[e, h], at_g(1))

    def token_down(e, h):
        src = xv if e == 0 else tok.at[g + e]
        return copy(half(src, h), half(tok.at[g + e], h), td_s.at[e], td_r.at[e, h], at_g(n_g - 1))

    def token_start(e):
        for h in range(2):
            @pl.when((g >= e) & (g < n_g - 1))
            def _():
                if e > 0:
                    ref = half(tok.at[g - e], h)
                    copy(ref, ref, tu_s.at[e], tu_r.at[e - 1, h], at_g(1)).wait_recv()
                token_up(e, h).start()

            @pl.when((g <= n_g - 1 - e) & (g > 0))
            def _():
                if e > 0:
                    ref = half(tok.at[g + e], h)
                    copy(ref, ref, td_s.at[e], td_r.at[e - 1, h], at_g(n_g - 1)).wait_recv()
                token_down(e, h).start()

    def token_end():
        for e in hops:
            for h in range(2):
                @pl.when((g >= e) & (g == n_g - 1))
                def _():
                    ref = half(tok.at[g - e], h)
                    copy(ref, ref, tu_s.at[0], tu_r.at[e - 1, h], at_g(1)).wait_recv()

                @pl.when((g <= n_g - 1 - e) & (g == 0))
                def _():
                    ref = half(tok.at[g + e], h)
                    copy(ref, ref, td_s.at[0], td_r.at[e - 1, h], at_g(n_g - 1)).wait_recv()

    def bias(k, src, slot):
        return copy(src, ubf.at[slot], bs_s.at[slot], bs_r.at[slot], at_m(k))

    def upward(v, e):
        part = pl.ds(e + 1, n_g - 1 - e)
        return copy(pb.at[v, part], from_low.at[v, part], lo_s.at[0], lo_r.at[v], at_g(1))

    def downward(v, e):
        part = pl.ds(0, n_g - 1 - e)
        return copy(pb.at[v, part], from_high.at[v, part], hi_s.at[0], hi_r.at[v], at_g(n_g - 1))

    def piece_up(v, d):
        return copy(pb.at[v, d], from_low.at[v, d], lo_s.at[0], end_r.at[0, v - v_tail, d], at_g(1))

    def piece_down(v, d):
        return copy(pb.at[v, d], from_high.at[v, d], hi_s.at[0], end_r.at[1, v - v_tail, d], at_g(n_g - 1))

    def normalize(values, at):
        values = values.astype(jnp.float32)
        center = jnp.mean(values, axis=1, keepdims=True)
        spread = jnp.mean((values - center) ** 2, axis=1, keepdims=True)
        lines = (values - center) * lax.rsqrt(spread + 1e-05) * gain[...] + nbias[...]
        normed[pl.ds(pl.multiple_of(at * rows, rows), rows), :] = lines.astype(jnp.bfloat16)

    barrier = pltpu.get_barrier_semaphore()
    near = [at_x(k) for k in xs] + [at_m(k) for k in ms]
    if cores > 1:
        near.append(partner)

    def greet(device):
        pl.semaphore_signal(barrier, inc=1, device_id=device, device_id_type=MESH)

    for device in near:
        greet(device)

    @pl.when(g < n_g - 1)
    def _():
        greet(at_g(1))

    @pl.when(g > 0)
    def _():
        greet(at_g(n_g - 1))

    own_up = upf.at[m, pl.ds(pl.multiple_of(img * depth, depth), depth), :]
    loads = [pltpu.make_async_copy(a, b, in_sem.at[i]) for i, (a, b) in enumerate((
        (x_hbm, xv), (up_hbm, own_up), (gain_hbm, gain), (nbias_hbm, nbias), (ubias_hbm, ubias), (dbias_hbm, dbias)))]
    for i in (1, 0, 2, 3, 4, 5):
        loads[i].start()
    loads[1].wait()
    ends = (g + n_g - 1) // n_g + (2 * n_g - 2 - g) // n_g
    pl.semaphore_wait(barrier, len(near) + ends)

    for s in range(UP_STAGES):
        issue(s)
    loads[0].wait()
    if n_g > 1:
        token_start(0)
    for j in range(n_chunk):
        own_down(j).start()
    for i in (2, 3, 4, 5):
        loads[i].wait()
    for k in ms:
        bias(k, ubias, k - 1).start()
    normalize(xv[...], g)

    def up_rows(km, first, last):
        place = lax.rem(m - km + pair, pair)
        biases = ubias if km == 0 else ubf.at[km - 1]

        def up_tile(n, carry):
            cols = pl.ds(pl.multiple_of(n * TILE, TILE), TILE)
            summed = jnp.dot(normed[...], upf[place, :, cols], preferred_element_type=jnp.float32)
            at = pl.ds(pl.multiple_of(place * units + n * TILE, TILE), TILE)
            hidden[:, at] = jax.nn.gelu(summed + biases[:, cols]).astype(jnp.bfloat16)
            return carry

        lax.fori_loop(first, last, up_tile, 0)

    for s in range(max(UP_STAGES, n_g - 1)):
        if 0 < s + 1 < n_g - 1:
            token_start(s + 1)
        if s < UP_STAGES:
            forward_m(s)
            forward_x(s)
    own_down(0).wait()
    issue(UP_STAGES)
    if n_chunk > 1:
        own_down(1).wait()
        issue_m(UP_STAGES + 1)
    token_end()
    for k in hops:
        o = lax.rem(g + k, n_g)
        normalize(tok[o], o)
    for s in range(UP_STAGES):
        take_up(s, 0)
    up_rows(0, 0, n_tile)
    for s in range(UP_STAGES):
        for k in xs:
            collect(s, k)
    for km in ms:
        bias(km, ubias, km - 1).wait_recv()
        for s in range(UP_STAGES):
            take_up(s, km)
        up_rows(km, 0, n_tile // 2)
        if km == pair - 1:
            forward_m(UP_STAGES)
            if n_chunk > 1:
                issue_x(UP_STAGES + 1)
        up_rows(km, n_tile // 2, n_tile)
    if pair == 1 and n_chunk > 1:
        issue_x(UP_STAGES + 1)

    def multiply(v, j, k):
        value = jnp.dot(hidden[...], dn[j * n_x + x_from(k)], preferred_element_type=jnp.float32)
        pb[v] = value.reshape(n_g, rows, wide).astype(jnp.bfloat16)

    upper = 2 * g // n_g
    far_d = (1 - upper) * (n_g - 1)

    def multiply_far(v, j, k):
        lines = hidden[pl.ds(pl.multiple_of(far_d * rows, rows), rows), :]
        value = jnp.dot(lines, dn[j * n_x + x_from(k)], preferred_element_type=jnp.float32)
        pb[v, far_d] = value.astype(jnp.bfloat16)

    def multiply_rest(v, j, k):
        if n_g > 1:
            lines = hidden[pl.ds(pl.multiple_of(upper * rows, rows), (n_g - 1) * rows), :]
            value = jnp.dot(lines, dn[j * n_x + x_from(k)], preferred_element_type=jnp.float32)
            pb[v, pl.ds(upper, n_g - 1)] = value.reshape(n_g - 1, rows, wide).astype(jnp.bfloat16)

    def add(v, part, arrived):
        pb[v, part] = (pb[v, part].astype(jnp.float32) + arrived[v, part].astype(jnp.float32)).astype(jnp.bfloat16)

    def pass_on(step):
        for e in reversed(range(n_g - 1)):
            v = step - LAG * e

            @pl.when((g == e) & (v >= 0) & (v < v_tail))
            def _():
                if e > 0:
                    upward(v, e - 1).wait_recv()
                    add(v, pl.ds(e + 1, n_g - 1 - e), from_low)
                upward(v, e).start()

            @pl.when((g == n_g - 1 - e) & (v >= 0) & (v < v_tail))
            def _():
                if e > 0:
                    downward(v, e - 1).wait_recv()
                    add(v, pl.ds(0, n_g - 1 - e), from_high)
                downward(v, e).start()

    def pass_pieces(step, first, stop):
        for e in reversed(range(n_g - 1)):
            v = step - LAG * e
            for i in range(first, min(stop, n_g - 1 - e)):
                for here, d, piece, arrived in (
                        (e, n_g - 1 - i, piece_up, from_low), (n_g - 1 - e, i, piece_down, from_high)):
                    @pl.when((g == here) & (v >= v_tail) & (v < n_v))
                    def _():
                        if e > 0:
                            piece(v, d).wait_recv()
                            add(v, d, arrived)
                        piece(v, d).start()

    def pass_far(step):
        pass_on(step)
        pass_pieces(step, 0, 1)

    def pass_near(step):
        pass_pieces(step, 1, n_g)

    def reduce(v):
        some = (v + n_v - 1) // n_v
        i = (v + n_x - 1) // n_x
        k = lax.rem(v + n_x - 1, n_x) * some + i // n_chunk
        j = i - (k + n_x - 1) // n_x
        for d in range(n_g):
            @pl.when(g == d)
            def _():
                if isinstance(v, int) and v >= v_tail:
                    if d > 0:
                        piece_up(v, d).wait_recv()
                    if d < n_g - 1:
                        piece_down(v, d).wait_recv()
                elif n_g > 1:
                    if d == n_g - 1:
                        upward(v, d - 1).wait_recv()
                    if d == 0:
                        downward(v, n_g - 2).wait_recv()

        src_x = x_from(k)
        for core in range(cores):
            cols = pl.ds(pl.multiple_of(((src_x * cores + core) * n_chunk + j) * LANES, LANES), LANES)
            piece = slice(core * LANES, (core + 1) * LANES)
            total = pb[v, g, :, piece].astype(jnp.float32) + dbias[:, cols]
            below = from_low[v, g, :, piece].astype(jnp.float32)
            above = from_high[v, g, :, piece].astype(jnp.float32)
            total = total + jnp.where(g > 0, below, 0.0) + jnp.where(g < n_g - 1, above, 0.0)
            out_ref[:, cols] = total.astype(jnp.bfloat16)

    settle = LAG * (n_g - 1) + 1

    def settled(v):
        @pl.when(v >= settle)
        def _():
            reduce(v - settle)

    def unit(v, j, k):
        take(j + UP_STAGES, k)
        multiply(v, j, k)
        pass_far(v)

        @pl.when(v < n_v - 2)
        def _():
            pass_near(v)

        settled(v)

    def last_unit(j, k):
        take(j + UP_STAGES, k)
        multiply_far(v_last, j, k)
        pass_far(v_last)
        multiply_rest(v_last, j, k)
        settled(v_last)

    def later(i, base, stop):
        def one(k, carry):
            collect(i + UP_STAGES, k)
            unit(base + k, i, k)
            return carry

        lax.fori_loop(1, stop, one, 0)

    def start(i):
        @pl.when(i + 2 < n_chunk)
        def _():
            own_down(i + 2).wait()
            issue(i + 2 + UP_STAGES)

    def tick(i, carry):
        forward_m(i + UP_STAGES)
        unit(n_x * (i - 1) + 1, i, 0)
        forward_x(i + UP_STAGES)
        start(i)
        later(i - 1, n_x * (i - 1) + 1, n_x)
        return carry

    unit(0, 0, 0)
    forward_x(UP_STAGES)
    start(0)
    if n_x > 1 and n_chunk > 1:
        forward_m(1 + UP_STAGES)
        unit(1, 1, 0)
        for k in xs:
            collect(UP_STAGES, k)
        forward_x(1 + UP_STAGES)
        start(1)
        for k in xs:
            unit(1 + k, 0, k)
        lax.fori_loop(2, n_chunk, tick, 0)
        later(n_chunk - 1, n_x * (n_chunk - 1), n_x - 1)
        collect(n_chunk - 1 + UP_STAGES, n_x - 1)
        last_unit(n_chunk - 1, n_x - 1)
    else:
        lax.fori_loop(1, n_chunk - 1, tick, 0)
        forward_m(n_chunk - 1 + UP_STAGES)
        forward_x(n_chunk - 1 + UP_STAGES)
        last_unit(n_chunk - 1, 0)

    def drain(step, carry):
        pass_far(step)
        pass_near(step - 2)
        return carry

    def reduce_tick(v, carry):
        reduce(v)
        return carry

    lax.fori_loop(n_v, n_v + LAG * (n_g - 2) + 2, drain, 0)
    lax.fori_loop(max(n_v - settle, 0), v_tail, reduce_tick, 0)
    for v in range(v_tail, n_v):
        reduce(v)

    for t in range(2):
        s = 0 if t == 0 else UP_STAGES
        cut = low_part[t]

        def span(size):
            if t == 0:
                return upf.at[0, pl.ds(0, UP_STAGES * size), :]
            return dn.at[pl.ds(0, n_chunk), pl.ds(0, size), pl.ds(0, LANES)]

        full = u_rows if t == 0 else units
        for k in xs:
            direct_x(s, k, span(full)).wait_send()
        for k in ms:
            direct_m(s, k, span(full)).wait_send()
        for k in xs:
            for km in ms:
                relay_m(s, k, km, span(cut)).wait_send()
                relay_x(s, k, km, span(full - cut)).wait_send()
        if cores > 1:
            ref = upf.at[:, pl.ds(0, n_x * depth), :] if t == 0 else dn.at[:, :, pl.ds(0, LANES)]
            across(s, 0, 0, ref).wait_send()
    for e in range(n_g - 1):
        @pl.when(g == e)
        def _():
            ref = pb.at[:, pl.ds(e + 1, n_g - 1 - e)]
            copy(ref, ref, lo_s.at[0], lo_r.at[0], at_g(1)).wait_send()

        @pl.when(g == n_g - 1 - e)
        def _():
            ref = pb.at[:, pl.ds(0, n_g - 1 - e)]
            copy(ref, ref, hi_s.at[0], hi_r.at[0], at_g(n_g - 1)).wait_send()
    for e in range(n_g - 1):
        @pl.when((g >= e) & (g < n_g - 1))
        def _():
            copy(tok.at[0], tok.at[0], tu_s.at[e], tu_r.at[e, 0], at_g(1)).wait_send()

        @pl.when((g <= n_g - 1 - e) & (g > 0))
        def _():
            copy(tok.at[0], tok.at[0], td_s.at[e], td_r.at[e, 0], at_g(n_g - 1)).wait_send()
    for k in ms:
        bias(k, ubias, k - 1).wait_send()


def solution(mesh):
    n_img, n_tp = mesh.shape["img"], mesh.shape["tp"]
    cores = 2 if n_img % 2 == 0 else 1
    pair = 2 if n_tp % 2 == 0 else 1
    n_x, n_g = n_img // cores, n_tp // pair

    def on_device(x, gain, nbias, up, ubias, down, dbias):
        rows, width = x.shape
        depth, units = up.shape
        n_chunk = down.shape[1] // LANES
        stages = UP_STAGES + n_chunk
        n_v, wide = n_chunk * n_x, cores * LANES
        out_width = n_img * down.shape[1]
        bf16, f32 = jnp.bfloat16, jnp.float32
        dma = pltpu.SemaphoreType.DMA
        ox, om, og = max(n_x - 1, 1), max(pair - 1, 1), max(n_g - 1, 1)
        scratch = [
            pltpu.VMEM((rows, width), bf16),
            pltpu.VMEM((1, width), f32),
            pltpu.VMEM((1, width), f32),
            pltpu.VMEM((1, units), f32),
            pltpu.VMEM((1, out_width), f32),
            pltpu.VMEM((n_g, rows, width), bf16),
            pltpu.VMEM((n_g * rows, width), bf16),
            pltpu.VMEM((pair, width, units), bf16),
            pltpu.VMEM((om, 1, units), f32),
            pltpu.VMEM((n_g * rows, pair * units), bf16),
            pltpu.VMEM((n_v, pair * units, wide), bf16),
            pltpu.VMEM((n_v, n_g, rows, wide), bf16),
            pltpu.VMEM((n_v, n_g, rows, wide), bf16),
            pltpu.VMEM((n_v, n_g, rows, wide), bf16),
        ]
        scratch += [dma((6,)), dma((n_chunk,))]
        scratch += [dma((og,)), dma((og, 2))] * 2 + [dma((om,))] * 2
        scratch += [dma((2, ox)), dma((stages, ox)), dma((2, om)), dma((stages, om))]
        scratch += [dma((2, ox, om)), dma((stages, ox, om))] * 2
        scratch += [dma((2,)), dma((stages, max(n_x, pair)))]
        scratch += [dma((1,)), dma((n_v,))] * 2 + [dma((2, TAIL, n_g))]
        return pl.pallas_call(
            functools.partial(kernel, n_img, n_tp),
            out_shape=pltpu.VMEM((rows, out_width), bf16),
            in_specs=[pl.BlockSpec(memory_space=pl.ANY)] * 7,
            out_specs=pl.BlockSpec(memory_space=pltpu.VMEM),
            scratch_shapes=scratch,
            compiler_params=pltpu.CompilerParams(
                collective_id=0, has_side_effects=True, vmem_limit_bytes=60 * 1024 * 1024),
        )(x, gain.reshape(1, -1), nbias.reshape(1, -1), up, ubias.reshape(1, -1), down,
          dbias.reshape(1, -1))

    return jax.shard_map(
        on_device,
        mesh=mesh,
        in_specs=(P(("img", "tp"), None), P(), P(), P("img", "tp"), P("tp"), P("tp", "img"), P()),
        out_specs=P(("img", "tp"), None),
        check_vma=False,
    )
```

```python
import functools

import jax
import jax.numpy as jnp
from jax import lax
from jax.experimental import pallas as pl
from jax.experimental.pallas import tpu as pltpu
from jax.sharding import PartitionSpec as P

MESH = pl.DeviceIdType.MESH
LANES = 128
UP_STAGES = 2
LAG = 2
TILE = 256
TAIL = 3


def portion(size, num, den):
    return max(size * num // den // 16 * 16, 16)


def kernel(n_img, n_tp, x_hbm, gain_hbm, nbias_hbm, up_hbm, ubias_hbm, down_hbm, dbias_hbm, out_ref,
           xv, gain, nbias, ubias, dbias, tok, normed, upf, ubf, hidden, dn, pb, from_low, from_high,
           in_sem, own_sem, tu_s, tu_r, td_s, td_r, bs_s, bs_r,
           dx_s, dx_r, dm_s, dm_r, r1_s, r1_r, r2_s, r2_r, p_s, p_r, lo_s, lo_r, hi_s, hi_r, end_r):
    cores = 2 if n_img % 2 == 0 else 1
    pair = 2 if n_tp % 2 == 0 else 1
    n_x, n_g = n_img // cores, n_tp // pair
    img, tp = lax.axis_index("img"), lax.axis_index("tp")
    x, c = img // cores, img % cores
    g, m = tp // pair, tp % pair
    rows, width = xv.shape
    depth, units = up_hbm.shape
    n_chunk = down_hbm.shape[1] // LANES
    u_rows = depth // UP_STAGES
    stages = UP_STAGES + n_chunk
    wide = cores * LANES
    n_v = n_chunk * n_x
    v_last, v_tail = n_v - 1, n_v - TAIL
    xs, ms, hops = range(1, n_x), range(1, pair), range(1, n_g)
    n_tile = units // TILE
    low_part = portion(u_rows, 1, 4), portion(units, 9, 16)

    def at_x(k):
        return {"img": lax.rem(x + k, n_x) * cores + c, "tp": tp}

    def at_m(k):
        return {"img": img, "tp": g * pair + lax.rem(m + k, pair)}

    def at_g(k):
        return {"img": img, "tp": lax.rem(g + k, n_g) * pair + m}

    partner = {"img": x * cores + (cores - 1 - c), "tp": tp}

    def is_up(s):
        return isinstance(s, int) and s < UP_STAGES

    def kind(s):
        return 0 if is_up(s) else 1

    def x_from(k):
        return lax.rem(x - k + n_x, n_x)

    def block(s, kx, km, core, part=None):
        src_x = x_from(kx)
        src_m = lax.rem(m - km + pair, pair)
        size = u_rows if is_up(s) else units
        cut = low_part[kind(s)]
        off, size = {None: (0, size), 0: (0, cut), 1: (cut, size - cut)}[part]
        if is_up(s):
            lo = (src_x * cores + core) * depth + s * u_rows + off
            return upf.at[src_m, pl.ds(pl.multiple_of(lo, 16), size), :]
        lo = src_m * units + off
        return dn.at[(s - UP_STAGES) * n_x + src_x, pl.ds(pl.multiple_of(lo, 16), size),
                     pl.ds(pl.multiple_of(core * LANES, LANES), LANES)]

    def copy(src, dst, send, recv, device):
        return pltpu.make_async_remote_copy(
            src_ref=src, dst_ref=dst, send_sem=send, recv_sem=recv,
            device_id=device, device_id_type=MESH)

    def direct_x(s, k, ref):
        return copy(ref, ref, dx_s.at[kind(s), k - 1], dx_r.at[s, k - 1], at_x(k))

    def direct_m(s, k, ref):
        return copy(ref, ref, dm_s.at[kind(s), k - 1], dm_r.at[s, k - 1], at_m(k))

    def relay_m(s, kx, km, ref):
        return copy(ref, ref, r1_s.at[kind(s), kx - 1, km - 1], r1_r.at[s, kx - 1, km - 1], at_m(km))

    def relay_x(s, kx, km, ref):
        return copy(ref, ref, r2_s.at[kind(s), kx - 1, km - 1], r2_r.at[s, kx - 1, km - 1], at_x(kx))

    def across(s, kx, km, ref):
        return copy(ref, ref, p_s.at[kind(s)], p_r.at[s, km if is_up(s) else kx], partner)

    def issue_m(s):
        ref = block(s, 0, 0, c)
        for k in ms:
            direct_m(s, k, ref).start()
        if cores > 1:
            across(s, 0, 0, ref).start()

    def issue_x(s):
        ref = block(s, 0, 0, c)
        for k in xs:
            direct_x(s, k, ref).start()

    def issue(s):
        issue_m(s)
        issue_x(s)

    def forward_m(s):
        for km in ms:
            ref = block(s, 0, km, c)
            direct_m(s, km, ref).wait_recv()
            if cores > 1:
                across(s, 0, km, ref).start()
            for k in xs:
                relay_x(s, k, km, block(s, 0, km, c, 1)).start()

    def forward_x(s):
        for k in xs:
            ref = block(s, k, 0, c)
            direct_x(s, k, ref).wait_recv()
            for km in ms:
                relay_m(s, k, km, block(s, k, 0, c, 0)).start()
            if cores > 1:
                across(s, k, 0, ref).start()

    def collect(s, k):
        for km in ms:
            for part, relay in enumerate((relay_m, relay_x)):
                ref = block(s, k, km, c, part)
                relay(s, k, km, ref).wait_recv()
                if cores > 1:
                    across(s, k, km, ref).start()

    def take_up(s, km):
        if cores > 1:
            ref = upf.at[0, pl.ds(0, n_x * u_rows), :]
            across(s, 0, km, ref).wait_recv()

    def take(s, k):
        if cores > 1:
            ref = dn.at[(s - UP_STAGES) * n_x + x_from(k), :,
                        pl.ds(pl.multiple_of((cores - 1 - c) * LANES, LANES), LANES)]
            across(s, k, 0, ref).wait_recv()

    def own_down(j):
        return pltpu.make_async_copy(
            down_hbm.at[:, pl.ds(pl.multiple_of(j * LANES, LANES), LANES)],
            block(j + UP_STAGES, 0, 0, c), own_sem.at[j])

    def half(ref, h):
        return ref.at[pl.ds(h * (rows // 2), rows // 2), :]

    def token_up(e, h):
        src = xv if e == 0 else tok.at[g - e]
        return copy(half(src, h), half(tok.at[g - e], h), tu_s.at[e], tu_r.at[e, h], at_g(1))

    def token_down(e, h):
        src = xv if e == 0 else tok.at[g + e]
        return copy(half(src, h), half(tok.at[g + e], h), td_s.at[e], td_r.at[e, h], at_g(n_g - 1))

    def token_start(e):
        for h in range(2):
            @pl.when((g >= e) & (g < n_g - 1))
            def _():
                if e > 0:
                    ref = half(tok.at[g - e], h)
                    copy(ref, ref, tu_s.at[e], tu_r.at[e - 1, h], at_g(1)).wait_recv()
                token_up(e, h).start()

            @pl.when((g <= n_g - 1 - e) & (g > 0))
            def _():
                if e > 0:
                    ref = half(tok.at[g + e], h)
                    copy(ref, ref, td_s.at[e], td_r.at[e - 1, h], at_g(n_g - 1)).wait_recv()
                token_down(e, h).start()

    def token_end():
        for e in hops:
            for h in range(2):
                @pl.when((g >= e) & (g == n_g - 1))
                def _():
                    ref = half(tok.at[g - e], h)
                    copy(ref, ref, tu_s.at[0], tu_r.at[e - 1, h], at_g(1)).wait_recv()

                @pl.when((g <= n_g - 1 - e) & (g == 0))
                def _():
                    ref = half(tok.at[g + e], h)
                    copy(ref, ref, td_s.at[0], td_r.at[e - 1, h], at_g(n_g - 1)).wait_recv()

    def bias(k, src, slot):
        return copy(src, ubf.at[slot], bs_s.at[slot], bs_r.at[slot], at_m(k))

    def upward(v, e):
        part = pl.ds(e + 1, n_g - 1 - e)
        return copy(pb.at[v, part], from_low.at[v, part], lo_s.at[0], lo_r.at[v], at_g(1))

    def downward(v, e):
        part = pl.ds(0, n_g - 1 - e)
        return copy(pb.at[v, part], from_high.at[v, part], hi_s.at[0], hi_r.at[v], at_g(n_g - 1))

    def slab(d, h):
        if h is None:
            return d
        return d, pl.ds(h * (rows // 2), rows // 2)

    def piece_up(v, d, h):
        at = slab(d, h)
        at = (at,) if h is None else at
        return copy(pb.at[(v,) + at], from_low.at[(v,) + at], lo_s.at[0], end_r.at[0, v - v_tail, d if h != 1 else n_g], at_g(1))

    def piece_down(v, d, h):
        at = slab(d, h)
        at = (at,) if h is None else at
        return copy(pb.at[(v,) + at], from_high.at[(v,) + at], hi_s.at[0], end_r.at[1, v - v_tail, d if h != 1 else n_g],
                    at_g(n_g - 1))

    def normalize(values, at):
        values = values.astype(jnp.float32)
        center = jnp.mean(values, axis=1, keepdims=True)
        spread = jnp.mean((values - center) ** 2, axis=1, keepdims=True)
        lines = (values - center) * lax.rsqrt(spread + 1e-05) * gain[...] + nbias[...]
        normed[pl.ds(pl.multiple_of(at * rows, rows), rows), :] = lines.astype(jnp.bfloat16)

    barrier = pltpu.get_barrier_semaphore()
    near = [at_x(k) for k in xs] + [at_m(k) for k in ms]
    if cores > 1:
        near.append(partner)

    def greet(device):
        pl.semaphore_signal(barrier, inc=1, device_id=device, device_id_type=MESH)

    for device in near:
        greet(device)

    @pl.when(g < n_g - 1)
    def _():
        greet(at_g(1))

    @pl.when(g > 0)
    def _():
        greet(at_g(n_g - 1))

    own_up = upf.at[m, pl.ds(pl.multiple_of(img * depth, depth), depth), :]
    loads = [pltpu.make_async_copy(a, b, in_sem.at[i]) for i, (a, b) in enumerate((
        (x_hbm, xv), (up_hbm, own_up), (gain_hbm, gain), (nbias_hbm, nbias), (ubias_hbm, ubias), (dbias_hbm, dbias)))]
    for i in (1, 0, 2, 3, 4, 5):
        loads[i].start()
    loads[1].wait()
    ends = (g + n_g - 1) // n_g + (2 * n_g - 2 - g) // n_g
    pl.semaphore_wait(barrier, len(near) + ends)

    for s in range(UP_STAGES):
        issue(s)
    loads[0].wait()
    if n_g > 1:
        token_start(0)
    for j in range(n_chunk):
        own_down(j).start()
    for i in (2, 3, 4, 5):
        loads[i].wait()
    for k in ms:
        bias(k, ubias, k - 1).start()
    normalize(xv[...], g)

    def up_rows(km, first, last):
        place = lax.rem(m - km + pair, pair)
        biases = ubias if km == 0 else ubf.at[km - 1]

        def up_tile(n, carry):
            cols = pl.ds(pl.multiple_of(n * TILE, TILE), TILE)
            summed = jnp.dot(normed[...], upf[place, :, cols], preferred_element_type=jnp.float32)
            at = pl.ds(pl.multiple_of(place * units + n * TILE, TILE), TILE)
            hidden[:, at] = jax.nn.gelu(summed + biases[:, cols]).astype(jnp.bfloat16)
            return carry

        lax.fori_loop(first, last, up_tile, 0)

    for s in range(max(UP_STAGES, n_g - 1)):
        if 0 < s + 1 < n_g - 1:
            token_start(s + 1)
        if s < UP_STAGES:
            forward_m(s)
            forward_x(s)
    own_down(0).wait()
    issue(UP_STAGES)
    if n_chunk > 1:
        own_down(1).wait()
        issue_m(UP_STAGES + 1)
    token_end()
    for k in hops:
        o = lax.rem(g + k, n_g)
        normalize(tok[o], o)
    for s in range(UP_STAGES):
        take_up(s, 0)
    up_rows(0, 0, n_tile)
    for s in range(UP_STAGES):
        for k in xs:
            collect(s, k)
    for km in ms:
        bias(km, ubias, km - 1).wait_recv()
        for s in range(UP_STAGES):
            take_up(s, km)
        up_rows(km, 0, n_tile // 2)
        if km == pair - 1:
            forward_m(UP_STAGES)
            if n_chunk > 1:
                issue_x(UP_STAGES + 1)
        up_rows(km, n_tile // 2, n_tile)
    if pair == 1 and n_chunk > 1:
        issue_x(UP_STAGES + 1)

    def multiply(v, j, k):
        value = jnp.dot(hidden[...], dn[j * n_x + x_from(k)], preferred_element_type=jnp.float32)
        pb[v] = value.reshape(n_g, rows, wide).astype(jnp.bfloat16)

    upper = 2 * g // n_g
    far_d = (1 - upper) * (n_g - 1)

    def multiply_far(v, j, k):
        lines = hidden[pl.ds(pl.multiple_of(far_d * rows, rows), rows), :]
        value = jnp.dot(lines, dn[j * n_x + x_from(k)], preferred_element_type=jnp.float32)
        pb[v, far_d] = value.astype(jnp.bfloat16)

    def multiply_rest(v, j, k):
        if n_g > 1:
            lines = hidden[pl.ds(pl.multiple_of(upper * rows, rows), (n_g - 1) * rows), :]
            value = jnp.dot(lines, dn[j * n_x + x_from(k)], preferred_element_type=jnp.float32)
            pb[v, pl.ds(upper, n_g - 1)] = value.reshape(n_g - 1, rows, wide).astype(jnp.bfloat16)

    def add(v, part, arrived):
        at = (v,) + part if isinstance(part, tuple) else (v, part)
        pb[at] = (pb[at].astype(jnp.float32) + arrived[at].astype(jnp.float32)).astype(jnp.bfloat16)

    def pass_on(step):
        for e in reversed(range(n_g - 1)):
            v = step - LAG * e

            @pl.when((g == e) & (v >= 0) & (v < v_tail))
            def _():
                if e > 0:
                    upward(v, e - 1).wait_recv()
                    add(v, pl.ds(e + 1, n_g - 1 - e), from_low)
                upward(v, e).start()

            @pl.when((g == n_g - 1 - e) & (v >= 0) & (v < v_tail))
            def _():
                if e > 0:
                    downward(v, e - 1).wait_recv()
                    add(v, pl.ds(0, n_g - 1 - e), from_high)
                downward(v, e).start()

    def pass_pieces(step, first, stop):
        for e in reversed(range(n_g - 1)):
            v = step - LAG * e
            for i in range(first, min(stop, n_g - 1 - e)):
                for here, d, piece, arrived in (
                        (e, n_g - 1 - i, piece_up, from_low), (n_g - 1 - e, i, piece_down, from_high)):
                    @pl.when((g == here) & (v >= v_tail) & (v < n_v))
                    def _():
                        for h in (0, 1) if i == 0 else (None,):
                            if e > 0:
                                piece(v, d, h).wait_recv()
                                add(v, slab(d, h), arrived)
                            piece(v, d, h).start()

    def pass_far(step):
        pass_on(step)
        pass_pieces(step, 0, 1)

    def pass_near(step):
        pass_pieces(step, 1, n_g)

    def reduce(v):
        some = (v + n_v - 1) // n_v
        i = (v + n_x - 1) // n_x
        k = lax.rem(v + n_x - 1, n_x) * some + i // n_chunk
        j = i - (k + n_x - 1) // n_x
        for d in range(n_g):
            @pl.when(g == d)
            def _():
                if isinstance(v, int) and v >= v_tail:
                    if d > 0:
                        for h in (0, 1) if d == n_g - 1 else (None,):
                            piece_up(v, d, h).wait_recv()
                    if d < n_g - 1:
                        for h in (0, 1) if d == 0 else (None,):
                            piece_down(v, d, h).wait_recv()
                elif n_g > 1:
                    if d == n_g - 1:
                        upward(v, d - 1).wait_recv()
                    if d == 0:
                        downward(v, n_g - 2).wait_recv()

        src_x = x_from(k)
        for core in range(cores):
            cols = pl.ds(pl.multiple_of(((src_x * cores + core) * n_chunk + j) * LANES, LANES), LANES)
            piece = slice(core * LANES, (core + 1) * LANES)
            total = pb[v, g, :, piece].astype(jnp.float32) + dbias[:, cols]
            below = from_low[v, g, :, piece].astype(jnp.float32)
            above = from_high[v, g, :, piece].astype(jnp.float32)
            total = total + jnp.where(g > 0, below, 0.0) + jnp.where(g < n_g - 1, above, 0.0)
            out_ref[:, cols] = total.astype(jnp.bfloat16)

    settle = LAG * (n_g - 1) + 1

    def settled(v):
        @pl.when(v >= settle)
        def _():
            reduce(v - settle)

    def unit(v, j, k):
        take(j + UP_STAGES, k)
        multiply(v, j, k)
        pass_far(v)

        @pl.when(v < n_v - 2)
        def _():
            pass_near(v)

        settled(v)

    def last_unit(j, k):
        take(j + UP_STAGES, k)
        multiply_far(v_last, j, k)
        pass_far(v_last)
        multiply_rest(v_last, j, k)
        settled(v_last)

    def later(i, base, stop):
        def one(k, carry):
            collect(i + UP_STAGES, k)
            unit(base + k, i, k)
            return carry

        lax.fori_loop(1, stop, one, 0)

    def start(i):
        @pl.when(i + 2 < n_chunk)
        def _():
            own_down(i + 2).wait()
            issue(i + 2 + UP_STAGES)

    def tick(i, carry):
        forward_m(i + UP_STAGES)
        unit(n_x * (i - 1) + 1, i, 0)
        forward_x(i + UP_STAGES)
        start(i)
        later(i - 1, n_x * (i - 1) + 1, n_x)
        return carry

    unit(0, 0, 0)
    forward_x(UP_STAGES)
    start(0)
    if n_x > 1 and n_chunk > 1:
        forward_m(1 + UP_STAGES)
        unit(1, 1, 0)
        for k in xs:
            collect(UP_STAGES, k)
        forward_x(1 + UP_STAGES)
        start(1)
        for k in xs:
            unit(1 + k, 0, k)
        lax.fori_loop(2, n_chunk, tick, 0)
        later(n_chunk - 1, n_x * (n_chunk - 1), n_x - 1)
        collect(n_chunk - 1 + UP_STAGES, n_x - 1)
        last_unit(n_chunk - 1, n_x - 1)
    else:
        lax.fori_loop(1, n_chunk - 1, tick, 0)
        forward_m(n_chunk - 1 + UP_STAGES)
        forward_x(n_chunk - 1 + UP_STAGES)
        last_unit(n_chunk - 1, 0)

    def drain(step, carry):
        pass_far(step)
        pass_near(step - 2)
        return carry

    def reduce_tick(v, carry):
        reduce(v)
        return carry

    lax.fori_loop(n_v, n_v + LAG * (n_g - 2) + 2, drain, 0)
    lax.fori_loop(max(n_v - settle, 0), v_tail, reduce_tick, 0)
    for v in range(v_tail, n_v):
        reduce(v)

    for t in range(2):
        s = 0 if t == 0 else UP_STAGES
        cut = low_part[t]

        def span(size):
            if t == 0:
                return upf.at[0, pl.ds(0, UP_STAGES * size), :]
            return dn.at[pl.ds(0, n_chunk), pl.ds(0, size), pl.ds(0, LANES)]

        full = u_rows if t == 0 else units
        for k in xs:
            direct_x(s, k, span(full)).wait_send()
        for k in ms:
            direct_m(s, k, span(full)).wait_send()
        for k in xs:
            for km in ms:
                relay_m(s, k, km, span(cut)).wait_send()
                relay_x(s, k, km, span(full - cut)).wait_send()
        if cores > 1:
            ref = upf.at[:, pl.ds(0, n_x * depth), :] if t == 0 else dn.at[:, :, pl.ds(0, LANES)]
            across(s, 0, 0, ref).wait_send()
    for e in range(n_g - 1):
        @pl.when(g == e)
        def _():
            ref = pb.at[:, pl.ds(e + 1, n_g - 1 - e)]
            copy(ref, ref, lo_s.at[0], lo_r.at[0], at_g(1)).wait_send()

        @pl.when(g == n_g - 1 - e)
        def _():
            ref = pb.at[:, pl.ds(0, n_g - 1 - e)]
            copy(ref, ref, hi_s.at[0], hi_r.at[0], at_g(n_g - 1)).wait_send()
    for e in range(n_g - 1):
        @pl.when((g >= e) & (g < n_g - 1))
        def _():
            copy(tok.at[0], tok.at[0], tu_s.at[e], tu_r.at[e, 0], at_g(1)).wait_send()

        @pl.when((g <= n_g - 1 - e) & (g > 0))
        def _():
            copy(tok.at[0], tok.at[0], td_s.at[e], td_r.at[e, 0], at_g(n_g - 1)).wait_send()
    for k in ms:
        bias(k, ubias, k - 1).wait_send()


def solution(mesh):
    n_img, n_tp = mesh.shape["img"], mesh.shape["tp"]
    cores = 2 if n_img % 2 == 0 else 1
    pair = 2 if n_tp % 2 == 0 else 1
    n_x, n_g = n_img // cores, n_tp // pair

    def on_device(x, gain, nbias, up, ubias, down, dbias):
        rows, width = x.shape
        depth, units = up.shape
        n_chunk = down.shape[1] // LANES
        stages = UP_STAGES + n_chunk
        n_v, wide = n_chunk * n_x, cores * LANES
        out_width = n_img * down.shape[1]
        bf16, f32 = jnp.bfloat16, jnp.float32
        dma = pltpu.SemaphoreType.DMA
        ox, om, og = max(n_x - 1, 1), max(pair - 1, 1), max(n_g - 1, 1)
        scratch = [
            pltpu.VMEM((rows, width), bf16),
            pltpu.VMEM((1, width), f32),
            pltpu.VMEM((1, width), f32),
            pltpu.VMEM((1, units), f32),
            pltpu.VMEM((1, out_width), f32),
            pltpu.VMEM((n_g, rows, width), bf16),
            pltpu.VMEM((n_g * rows, width), bf16),
            pltpu.VMEM((pair, width, units), bf16),
            pltpu.VMEM((om, 1, units), f32),
            pltpu.VMEM((n_g * rows, pair * units), bf16),
            pltpu.VMEM((n_v, pair * units, wide), bf16),
            pltpu.VMEM((n_v, n_g, rows, wide), bf16),
            pltpu.VMEM((n_v, n_g, rows, wide), bf16),
            pltpu.VMEM((n_v, n_g, rows, wide), bf16),
        ]
        scratch += [dma((6,)), dma((n_chunk,))]
        scratch += [dma((og,)), dma((og, 2))] * 2 + [dma((om,))] * 2
        scratch += [dma((2, ox)), dma((stages, ox)), dma((2, om)), dma((stages, om))]
        scratch += [dma((2, ox, om)), dma((stages, ox, om))] * 2
        scratch += [dma((2,)), dma((stages, max(n_x, pair)))]
        scratch += [dma((1,)), dma((n_v,))] * 2 + [dma((2, TAIL, n_g + 1))]
        return pl.pallas_call(
            functools.partial(kernel, n_img, n_tp),
            out_shape=pltpu.VMEM((rows, out_width), bf16),
            in_specs=[pl.BlockSpec(memory_space=pl.ANY)] * 7,
            out_specs=pl.BlockSpec(memory_space=pltpu.VMEM),
            scratch_shapes=scratch,
            compiler_params=pltpu.CompilerParams(
                collective_id=0, has_side_effects=True, vmem_limit_bytes=60 * 1024 * 1024),
        )(x, gain.reshape(1, -1), nbias.reshape(1, -1), up, ubias.reshape(1, -1), down,
          dbias.reshape(1, -1))

    return jax.shard_map(
        on_device,
        mesh=mesh,
        in_specs=(P(("img", "tp"), None), P(), P(), P("img", "tp"), P("tp"), P("tp", "img"), P()),
        out_specs=P(("img", "tp"), None),
        check_vma=False,
    )
```

```python
import functools

import jax
import jax.numpy as jnp
from jax import lax
from jax.experimental import pallas as pl
from jax.experimental.pallas import tpu as pltpu
from jax.sharding import PartitionSpec as P

MESH = pl.DeviceIdType.MESH
LANES = 128
UP_STAGES = 2
LAG = 2
TILE = 256
TAIL = 3


def portion(size, num, den):
    return max(size * num // den // 16 * 16, 16)


def kernel(n_img, n_tp, x_hbm, gain_hbm, nbias_hbm, up_hbm, ubias_hbm, down_hbm, dbias_hbm, out_ref,
           xv, gain, nbias, ubias, dbias, tok, normed, upf, ubf, hidden, dn, pb, from_low, from_high,
           in_sem, own_sem, tu_s, tu_r, td_s, td_r, bs_s, bs_r,
           dx_s, dx_r, dm_s, dm_r, r1_s, r1_r, r2_s, r2_r, p_s, p_r, lo_s, lo_r, hi_s, hi_r, end_r):
    cores = 2 if n_img % 2 == 0 else 1
    pair = 2 if n_tp % 2 == 0 else 1
    n_x, n_g = n_img // cores, n_tp // pair
    img, tp = lax.axis_index("img"), lax.axis_index("tp")
    x, c = img // cores, img % cores
    g, m = tp // pair, tp % pair
    rows, width = xv.shape
    depth, units = up_hbm.shape
    n_chunk = down_hbm.shape[1] // LANES
    u_rows = depth // UP_STAGES
    stages = UP_STAGES + n_chunk
    wide = cores * LANES
    n_v = n_chunk * n_x
    v_last, v_tail = n_v - 1, n_v - TAIL
    xs, ms, hops = range(1, n_x), range(1, pair), range(1, n_g)
    n_tile = units // TILE
    low_part = portion(u_rows, 3, 8), portion(units, 17, 32)

    def at_x(k):
        return {"img": lax.rem(x + k, n_x) * cores + c, "tp": tp}

    def at_m(k):
        return {"img": img, "tp": g * pair + lax.rem(m + k, pair)}

    def at_g(k):
        return {"img": img, "tp": lax.rem(g + k, n_g) * pair + m}

    partner = {"img": x * cores + (cores - 1 - c), "tp": tp}

    def is_up(s):
        return isinstance(s, int) and s < UP_STAGES

    def kind(s):
        return 0 if is_up(s) else 1

    def x_from(k):
        return lax.rem(x - k + n_x, n_x)

    def block(s, kx, km, core, part=None):
        src_x = x_from(kx)
        src_m = lax.rem(m - km + pair, pair)
        size = u_rows if is_up(s) else units
        cut = low_part[kind(s)]
        off, size = {None: (0, size), 0: (0, cut), 1: (cut, size - cut)}[part]
        if is_up(s):
            lo = (src_x * cores + core) * depth + s * u_rows + off
            return upf.at[src_m, pl.ds(pl.multiple_of(lo, 16), size), :]
        lo = src_m * units + off
        return dn.at[(s - UP_STAGES) * n_x + src_x, pl.ds(pl.multiple_of(lo, 16), size),
                     pl.ds(pl.multiple_of(core * LANES, LANES), LANES)]

    def copy(src, dst, send, recv, device):
        return pltpu.make_async_remote_copy(
            src_ref=src, dst_ref=dst, send_sem=send, recv_sem=recv,
            device_id=device, device_id_type=MESH)

    def direct_x(s, k, ref):
        return copy(ref, ref, dx_s.at[kind(s), k - 1], dx_r.at[s, k - 1], at_x(k))

    def direct_m(s, k, ref):
        return copy(ref, ref, dm_s.at[kind(s), k - 1], dm_r.at[s, k - 1], at_m(k))

    def relay_m(s, kx, km, ref):
        return copy(ref, ref, r1_s.at[kind(s), kx - 1, km - 1], r1_r.at[s, kx - 1, km - 1], at_m(km))

    def relay_x(s, kx, km, ref):
        return copy(ref, ref, r2_s.at[kind(s), kx - 1, km - 1], r2_r.at[s, kx - 1, km - 1], at_x(kx))

    def across(s, kx, km, ref):
        return copy(ref, ref, p_s.at[kind(s)], p_r.at[s, km if is_up(s) else kx], partner)

    def issue_m(s):
        ref = block(s, 0, 0, c)
        for k in ms:
            direct_m(s, k, ref).start()
        if cores > 1:
            across(s, 0, 0, ref).start()

    def issue_x(s):
        ref = block(s, 0, 0, c)
        for k in xs:
            direct_x(s, k, ref).start()

    def issue(s):
        issue_m(s)
        issue_x(s)

    def forward_m(s):
        for km in ms:
            ref = block(s, 0, km, c)
            direct_m(s, km, ref).wait_recv()
            if cores > 1:
                across(s, 0, km, ref).start()
            for k in xs:
                relay_x(s, k, km, block(s, 0, km, c, 1)).start()

    def forward_x(s):
        for k in xs:
            ref = block(s, k, 0, c)
            direct_x(s, k, ref).wait_recv()
            for km in ms:
                relay_m(s, k, km, block(s, k, 0, c, 0)).start()
            if cores > 1:
                across(s, k, 0, ref).start()

    def collect(s, k):
        for km in ms:
            for part, relay in enumerate((relay_m, relay_x)):
                ref = block(s, k, km, c, part)
                relay(s, k, km, ref).wait_recv()
                if cores > 1:
                    across(s, k, km, ref).start()

    def take_up(s, km):
        if cores > 1:
            ref = upf.at[0, pl.ds(0, n_x * u_rows), :]
            across(s, 0, km, ref).wait_recv()

    def take(s, k):
        if cores > 1:
            ref = dn.at[(s - UP_STAGES) * n_x + x_from(k), :,
                        pl.ds(pl.multiple_of((cores - 1 - c) * LANES, LANES), LANES)]
            across(s, k, 0, ref).wait_recv()

    def own_down(j):
        return pltpu.make_async_copy(
            down_hbm.at[:, pl.ds(pl.multiple_of(j * LANES, LANES), LANES)],
            block(j + UP_STAGES, 0, 0, c), own_sem.at[j])

    def half(ref, h):
        return ref.at[pl.ds(h * (rows // 2), rows // 2), :]

    def token_up(e, h):
        src = xv if e == 0 else tok.at[g - e]
        return copy(half(src, h), half(tok.at[g - e], h), tu_s.at[e], tu_r.at[e, h], at_g(1))

    def token_down(e, h):
        src = xv if e == 0 else tok.at[g + e]
        return copy(half(src, h), half(tok.at[g + e], h), td_s.at[e], td_r.at[e, h], at_g(n_g - 1))

    def token_start(e):
        for h in range(2):
            @pl.when((g >= e) & (g < n_g - 1))
            def _():
                if e > 0:
                    ref = half(tok.at[g - e], h)
                    copy(ref, ref, tu_s.at[e], tu_r.at[e - 1, h], at_g(1)).wait_recv()
                token_up(e, h).start()

            @pl.when((g <= n_g - 1 - e) & (g > 0))
            def _():
                if e > 0:
                    ref = half(tok.at[g + e], h)
                    copy(ref, ref, td_s.at[e], td_r.at[e - 1, h], at_g(n_g - 1)).wait_recv()
                token_down(e, h).start()

    def token_end():
        for e in hops:
            for h in range(2):
                @pl.when((g >= e) & (g == n_g - 1))
                def _():
                    ref = half(tok.at[g - e], h)
                    copy(ref, ref, tu_s.at[0], tu_r.at[e - 1, h], at_g(1)).wait_recv()

                @pl.when((g <= n_g - 1 - e) & (g == 0))
                def _():
                    ref = half(tok.at[g + e], h)
                    copy(ref, ref, td_s.at[0], td_r.at[e - 1, h], at_g(n_g - 1)).wait_recv()

    def bias(k, src, slot):
        return copy(src, ubf.at[slot], bs_s.at[slot], bs_r.at[slot], at_m(k))

    def upward(v, e):
        part = pl.ds(e + 1, n_g - 1 - e)
        return copy(pb.at[v, part], from_low.at[v, part], lo_s.at[0], lo_r.at[v], at_g(1))

    def downward(v, e):
        part = pl.ds(0, n_g - 1 - e)
        return copy(pb.at[v, part], from_high.at[v, part], hi_s.at[0], hi_r.at[v], at_g(n_g - 1))

    def slab(d, h):
        if h is None:
            return d
        return d, pl.ds(h * (rows // 2), rows // 2)

    def piece_up(v, d, h):
        at = slab(d, h)
        at = (at,) if h is None else at
        return copy(pb.at[(v,) + at], from_low.at[(v,) + at], lo_s.at[0], end_r.at[0, v - v_tail, d if h != 1 else n_g], at_g(1))

    def piece_down(v, d, h):
        at = slab(d, h)
        at = (at,) if h is None else at
        return copy(pb.at[(v,) + at], from_high.at[(v,) + at], hi_s.at[0], end_r.at[1, v - v_tail, d if h != 1 else n_g],
                    at_g(n_g - 1))

    def normalize(values, at):
        values = values.astype(jnp.float32)
        center = jnp.mean(values, axis=1, keepdims=True)
        spread = jnp.mean((values - center) ** 2, axis=1, keepdims=True)
        lines = (values - center) * lax.rsqrt(spread + 1e-05) * gain[...] + nbias[...]
        normed[pl.ds(pl.multiple_of(at * rows, rows), rows), :] = lines.astype(jnp.bfloat16)

    barrier = pltpu.get_barrier_semaphore()
    near = [at_x(k) for k in xs] + [at_m(k) for k in ms]
    if cores > 1:
        near.append(partner)

    def greet(device):
        pl.semaphore_signal(barrier, inc=1, device_id=device, device_id_type=MESH)

    for device in near:
        greet(device)

    @pl.when(g < n_g - 1)
    def _():
        greet(at_g(1))

    @pl.when(g > 0)
    def _():
        greet(at_g(n_g - 1))

    own_up = upf.at[m, pl.ds(pl.multiple_of(img * depth, depth), depth), :]
    loads = [pltpu.make_async_copy(a, b, in_sem.at[i]) for i, (a, b) in enumerate((
        (x_hbm, xv), (up_hbm, own_up), (gain_hbm, gain), (nbias_hbm, nbias), (ubias_hbm, ubias), (dbias_hbm, dbias)))]
    for i in (1, 0, 2, 3, 4, 5):
        loads[i].start()
    loads[1].wait()
    ends = (g + n_g - 1) // n_g + (2 * n_g - 2 - g) // n_g
    pl.semaphore_wait(barrier, len(near) + ends)

    for s in range(UP_STAGES):
        issue(s)
    loads[0].wait()
    if n_g > 1:
        token_start(0)
    for j in range(n_chunk):
        own_down(j).start()
    for i in (2, 3, 4, 5):
        loads[i].wait()
    for k in ms:
        bias(k, ubias, k - 1).start()
    normalize(xv[...], g)

    def up_rows(km, first, last):
        place = lax.rem(m - km + pair, pair)
        biases = ubias if km == 0 else ubf.at[km - 1]

        def up_tile(n, carry):
            cols = pl.ds(pl.multiple_of(n * TILE, TILE), TILE)
            summed = jnp.dot(normed[...], upf[place, :, cols], preferred_element_type=jnp.float32)
            at = pl.ds(pl.multiple_of(place * units + n * TILE, TILE), TILE)
            hidden[:, at] = jax.nn.gelu(summed + biases[:, cols]).astype(jnp.bfloat16)
            return carry

        lax.fori_loop(first, last, up_tile, 0)

    for s in range(max(UP_STAGES, n_g - 1)):
        if 0 < s + 1 < n_g - 1:
            token_start(s + 1)
        if s < UP_STAGES:
            forward_m(s)
            forward_x(s)
    own_down(0).wait()
    issue(UP_STAGES)
    if n_chunk > 1:
        own_down(1).wait()
        issue_m(UP_STAGES + 1)
    token_end()
    for k in hops:
        o = lax.rem(g + k, n_g)
        normalize(tok[o], o)
    for s in range(UP_STAGES):
        take_up(s, 0)
    up_rows(0, 0, n_tile)
    for s in range(UP_STAGES):
        for k in xs:
            collect(s, k)
    for km in ms:
        bias(km, ubias, km - 1).wait_recv()
        for s in range(UP_STAGES):
            take_up(s, km)
        up_rows(km, 0, n_tile // 2)
        if km == pair - 1:
            forward_m(UP_STAGES)
            if n_chunk > 1:
                issue_x(UP_STAGES + 1)
        up_rows(km, n_tile // 2, n_tile)
    if pair == 1 and n_chunk > 1:
        issue_x(UP_STAGES + 1)

    def multiply(v, j, k):
        value = jnp.dot(hidden[...], dn[j * n_x + x_from(k)], preferred_element_type=jnp.float32)
        pb[v] = value.reshape(n_g, rows, wide).astype(jnp.bfloat16)

    upper = 2 * g // n_g
    far_d = (1 - upper) * (n_g - 1)

    def multiply_far(v, j, k):
        lines = hidden[pl.ds(pl.multiple_of(far_d * rows, rows), rows), :]
        value = jnp.dot(lines, dn[j * n_x + x_from(k)], preferred_element_type=jnp.float32)
        pb[v, far_d] = value.astype(jnp.bfloat16)

    def multiply_rest(v, j, k):
        if n_g > 1:
            lines = hidden[pl.ds(pl.multiple_of(upper * rows, rows), (n_g - 1) * rows), :]
            value = jnp.dot(lines, dn[j * n_x + x_from(k)], preferred_element_type=jnp.float32)
            pb[v, pl.ds(upper, n_g - 1)] = value.reshape(n_g - 1, rows, wide).astype(jnp.bfloat16)

    def add(v, part, arrived):
        at = (v,) + part if isinstance(part, tuple) else (v, part)
        pb[at] = (pb[at].astype(jnp.float32) + arrived[at].astype(jnp.float32)).astype(jnp.bfloat16)

    def pass_on(step):
        for e in reversed(range(n_g - 1)):
            v = step - LAG * e

            @pl.when((g == e) & (v >= 0) & (v < v_tail))
            def _():
                if e > 0:
                    upward(v, e - 1).wait_recv()
                    add(v, pl.ds(e + 1, n_g - 1 - e), from_low)
                upward(v, e).start()

            @pl.when((g == n_g - 1 - e) & (v >= 0) & (v < v_tail))
            def _():
                if e > 0:
                    downward(v, e - 1).wait_recv()
                    add(v, pl.ds(0, n_g - 1 - e), from_high)
                downward(v, e).start()

    def pass_pieces(step, first, stop):
        for e in reversed(range(n_g - 1)):
            v = step - LAG * e
            for i in range(first, min(stop, n_g - 1 - e)):
                for here, d, piece, arrived in (
                        (e, n_g - 1 - i, piece_up, from_low), (n_g - 1 - e, i, piece_down, from_high)):
                    @pl.when((g == here) & (v >= v_tail) & (v < n_v))
                    def _():
                        for h in (0, 1) if i == 0 else (None,):
                            if e > 0:
                                piece(v, d, h).wait_recv()
                                add(v, slab(d, h), arrived)
                            piece(v, d, h).start()

    def pass_far(step):
        pass_on(step)
        pass_pieces(step, 0, 1)

    def pass_near(step):
        pass_pieces(step, 1, n_g)

    def reduce(v):
        some = (v + n_v - 1) // n_v
        i = (v + n_x - 1) // n_x
        k = lax.rem(v + n_x - 1, n_x) * some + i // n_chunk
        j = i - (k + n_x - 1) // n_x
        for d in range(n_g):
            @pl.when(g == d)
            def _():
                if isinstance(v, int) and v >= v_tail:
                    if d > 0:
                        for h in (0, 1) if d == n_g - 1 else (None,):
                            piece_up(v, d, h).wait_recv()
                    if d < n_g - 1:
                        for h in (0, 1) if d == 0 else (None,):
                            piece_down(v, d, h).wait_recv()
                elif n_g > 1:
                    if d == n_g - 1:
                        upward(v, d - 1).wait_recv()
                    if d == 0:
                        downward(v, n_g - 2).wait_recv()

        src_x = x_from(k)
        for core in range(cores):
            cols = pl.ds(pl.multiple_of(((src_x * cores + core) * n_chunk + j) * LANES, LANES), LANES)
            piece = slice(core * LANES, (core + 1) * LANES)
            total = pb[v, g, :, piece].astype(jnp.float32) + dbias[:, cols]
            below = from_low[v, g, :, piece].astype(jnp.float32)
            above = from_high[v, g, :, piece].astype(jnp.float32)
            total = total + jnp.where(g > 0, below, 0.0) + jnp.where(g < n_g - 1, above, 0.0)
            out_ref[:, cols] = total.astype(jnp.bfloat16)

    settle = LAG * (n_g - 1) + 1

    def settled(v):
        @pl.when(v >= settle)
        def _():
            reduce(v - settle)

    def unit(v, j, k):
        take(j + UP_STAGES, k)
        multiply(v, j, k)
        pass_far(v)

        @pl.when(v < n_v - 2)
        def _():
            pass_near(v)

        settled(v)

    def last_unit(j, k):
        take(j + UP_STAGES, k)
        multiply_far(v_last, j, k)
        pass_far(v_last)
        multiply_rest(v_last, j, k)
        settled(v_last)

    def later(i, base, stop):
        def one(k, carry):
            collect(i + UP_STAGES, k)
            unit(base + k, i, k)
            return carry

        lax.fori_loop(1, stop, one, 0)

    def start(i):
        @pl.when(i + 2 < n_chunk)
        def _():
            own_down(i + 2).wait()
            issue(i + 2 + UP_STAGES)

    def tick(i, carry):
        forward_m(i + UP_STAGES)
        forward_x(i + UP_STAGES)
        start(i)
        unit(n_x * (i - 1) + 1, i, 0)
        later(i - 1, n_x * (i - 1) + 1, n_x)
        return carry

    unit(0, 0, 0)
    forward_x(UP_STAGES)
    start(0)
    if n_x > 1 and n_chunk > 1:
        forward_m(1 + UP_STAGES)
        unit(1, 1, 0)
        for k in xs:
            collect(UP_STAGES, k)
        forward_x(1 + UP_STAGES)
        start(1)
        for k in xs:
            unit(1 + k, 0, k)
        lax.fori_loop(2, n_chunk, tick, 0)
        later(n_chunk - 1, n_x * (n_chunk - 1), n_x - 1)
        collect(n_chunk - 1 + UP_STAGES, n_x - 1)
        last_unit(n_chunk - 1, n_x - 1)
    else:
        lax.fori_loop(1, n_chunk - 1, tick, 0)
        forward_m(n_chunk - 1 + UP_STAGES)
        forward_x(n_chunk - 1 + UP_STAGES)
        last_unit(n_chunk - 1, 0)

    def drain(step, carry):
        pass_far(step)
        pass_near(step - 2)
        return carry

    def reduce_tick(v, carry):
        reduce(v)
        return carry

    lax.fori_loop(n_v, n_v + LAG * (n_g - 2) + 2, drain, 0)
    lax.fori_loop(max(n_v - settle, 0), v_tail, reduce_tick, 0)
    for v in range(v_tail, n_v):
        reduce(v)

    for t in range(2):
        s = 0 if t == 0 else UP_STAGES
        cut = low_part[t]

        def span(size):
            if t == 0:
                return upf.at[0, pl.ds(0, UP_STAGES * size), :]
            return dn.at[pl.ds(0, n_chunk), pl.ds(0, size), pl.ds(0, LANES)]

        full = u_rows if t == 0 else units
        for k in xs:
            direct_x(s, k, span(full)).wait_send()
        for k in ms:
            direct_m(s, k, span(full)).wait_send()
        for k in xs:
            for km in ms:
                relay_m(s, k, km, span(cut)).wait_send()
                relay_x(s, k, km, span(full - cut)).wait_send()
        if cores > 1:
            ref = upf.at[:, pl.ds(0, n_x * depth), :] if t == 0 else dn.at[:, :, pl.ds(0, LANES)]
            across(s, 0, 0, ref).wait_send()
    for e in range(n_g - 1):
        @pl.when(g == e)
        def _():
            ref = pb.at[:, pl.ds(e + 1, n_g - 1 - e)]
            copy(ref, ref, lo_s.at[0], lo_r.at[0], at_g(1)).wait_send()

        @pl.when(g == n_g - 1 - e)
        def _():
            ref = pb.at[:, pl.ds(0, n_g - 1 - e)]
            copy(ref, ref, hi_s.at[0], hi_r.at[0], at_g(n_g - 1)).wait_send()
    for e in range(n_g - 1):
        @pl.when((g >= e) & (g < n_g - 1))
        def _():
            copy(tok.at[0], tok.at[0], tu_s.at[e], tu_r.at[e, 0], at_g(1)).wait_send()

        @pl.when((g <= n_g - 1 - e) & (g > 0))
        def _():
            copy(tok.at[0], tok.at[0], td_s.at[e], td_r.at[e, 0], at_g(n_g - 1)).wait_send()
    for k in ms:
        bias(k, ubias, k - 1).wait_send()


def solution(mesh):
    n_img, n_tp = mesh.shape["img"], mesh.shape["tp"]
    cores = 2 if n_img % 2 == 0 else 1
    pair = 2 if n_tp % 2 == 0 else 1
    n_x, n_g = n_img // cores, n_tp // pair

    def on_device(x, gain, nbias, up, ubias, down, dbias):
        rows, width = x.shape
        depth, units = up.shape
        n_chunk = down.shape[1] // LANES
        stages = UP_STAGES + n_chunk
        n_v, wide = n_chunk * n_x, cores * LANES
        out_width = n_img * down.shape[1]
        bf16, f32 = jnp.bfloat16, jnp.float32
        dma = pltpu.SemaphoreType.DMA
        ox, om, og = max(n_x - 1, 1), max(pair - 1, 1), max(n_g - 1, 1)
        scratch = [
            pltpu.VMEM((rows, width), bf16),
            pltpu.VMEM((1, width), f32),
            pltpu.VMEM((1, width), f32),
            pltpu.VMEM((1, units), f32),
            pltpu.VMEM((1, out_width), f32),
            pltpu.VMEM((n_g, rows, width), bf16),
            pltpu.VMEM((n_g * rows, width), bf16),
            pltpu.VMEM((pair, width, units), bf16),
            pltpu.VMEM((om, 1, units), f32),
            pltpu.VMEM((n_g * rows, pair * units), bf16),
            pltpu.VMEM((n_v, pair * units, wide), bf16),
            pltpu.VMEM((n_v, n_g, rows, wide), bf16),
            pltpu.VMEM((n_v, n_g, rows, wide), bf16),
            pltpu.VMEM((n_v, n_g, rows, wide), bf16),
        ]
        scratch += [dma((6,)), dma((n_chunk,))]
        scratch += [dma((og,)), dma((og, 2))] * 2 + [dma((om,))] * 2
        scratch += [dma((2, ox)), dma((stages, ox)), dma((2, om)), dma((stages, om))]
        scratch += [dma((2, ox, om)), dma((stages, ox, om))] * 2
        scratch += [dma((2,)), dma((stages, max(n_x, pair)))]
        scratch += [dma((1,)), dma((max(n_v - TAIL, 1),))] * 2 + [dma((2, TAIL, n_g + 1))]
        return pl.pallas_call(
            functools.partial(kernel, n_img, n_tp),
            out_shape=pltpu.VMEM((rows, out_width), bf16),
            in_specs=[pl.BlockSpec(memory_space=pl.ANY)] * 7,
            out_specs=pl.BlockSpec(memory_space=pltpu.VMEM),
            scratch_shapes=scratch,
            compiler_params=pltpu.CompilerParams(
                collective_id=0, has_side_effects=True, vmem_limit_bytes=60 * 1024 * 1024),
        )(x, gain.reshape(1, -1), nbias.reshape(1, -1), up, ubias.reshape(1, -1), down,
          dbias.reshape(1, -1))

    return jax.shard_map(
        on_device,
        mesh=mesh,
        in_specs=(P(("img", "tp"), None), P(), P(), P("img", "tp"), P("tp"), P("tp", "img"), P()),
        out_specs=P(("img", "tp"), None),
        check_vma=False,
    )
```

```python
import functools

import jax
import jax.numpy as jnp
from jax import lax
from jax.experimental import pallas as pl
from jax.experimental.pallas import tpu as pltpu
from jax.sharding import PartitionSpec as P

MESH = pl.DeviceIdType.MESH
LANES = 128
UP_STAGES = 2
LAG = 2
TILE = 256
TAIL = 3


def portion(size, num, den):
    return max(size * num // den // 16 * 16, 16)


def kernel(n_img, n_tp, x_hbm, gain_hbm, nbias_hbm, up_hbm, ubias_hbm, down_hbm, dbias_hbm, out_ref,
           xv, gain, nbias, ubias, dbias, tok, normed, upf, ubf, hidden, dn, pb, from_low, from_high,
           in_sem, own_sem, tu_s, tu_r, td_s, td_r, bs_s, bs_r,
           dx_s, dx_r, dm_s, dm_r, r1_s, r1_r, r2_s, r2_r, p_s, p_r, lo_s, lo_r, hi_s, hi_r, end_r):
    cores = 2 if n_img % 2 == 0 else 1
    pair = 2 if n_tp % 2 == 0 else 1
    n_x, n_g = n_img // cores, n_tp // pair
    img, tp = lax.axis_index("img"), lax.axis_index("tp")
    x, c = img // cores, img % cores
    g, m = tp // pair, tp % pair
    rows, width = xv.shape
    depth, units = up_hbm.shape
    n_chunk = down_hbm.shape[1] // LANES
    u_rows = depth // UP_STAGES
    stages = UP_STAGES + n_chunk
    wide = cores * LANES
    n_v = n_chunk * n_x
    v_last, v_tail = n_v - 1, n_v - TAIL
    xs, ms, hops = range(1, n_x), range(1, pair), range(1, n_g)
    n_tile = units // TILE
    low_part = portion(u_rows, 3, 8), portion(units, 17, 32)

    def at_x(k):
        return {"img": lax.rem(x + k, n_x) * cores + c, "tp": tp}

    def at_m(k):
        return {"img": img, "tp": g * pair + lax.rem(m + k, pair)}

    def at_g(k):
        return {"img": img, "tp": lax.rem(g + k, n_g) * pair + m}

    partner = {"img": x * cores + (cores - 1 - c), "tp": tp}

    def is_up(s):
        return isinstance(s, int) and s < UP_STAGES

    def kind(s):
        return 0 if is_up(s) else 1

    def x_from(k):
        return lax.rem(x - k + n_x, n_x)

    def block(s, kx, km, core, part=None):
        src_x = x_from(kx)
        src_m = lax.rem(m - km + pair, pair)
        size = u_rows if is_up(s) else units
        cut = low_part[kind(s)]
        off, size = {None: (0, size), 0: (0, cut), 1: (cut, size - cut)}[part]
        if is_up(s):
            lo = (src_x * cores + core) * depth + s * u_rows + off
            return upf.at[src_m, pl.ds(pl.multiple_of(lo, 16), size), :]
        lo = src_m * units + off
        return dn.at[(s - UP_STAGES) * n_x + src_x, pl.ds(pl.multiple_of(lo, 16), size),
                     pl.ds(pl.multiple_of(core * LANES, LANES), LANES)]

    def copy(src, dst, send, recv, device):
        return pltpu.make_async_remote_copy(
            src_ref=src, dst_ref=dst, send_sem=send, recv_sem=recv,
            device_id=device, device_id_type=MESH)

    def direct_x(s, k, ref):
        return copy(ref, ref, dx_s.at[kind(s), k - 1], dx_r.at[s, k - 1], at_x(k))

    def direct_m(s, k, ref):
        return copy(ref, ref, dm_s.at[kind(s), k - 1], dm_r.at[s, k - 1], at_m(k))

    def relay_m(s, kx, km, ref):
        return copy(ref, ref, r1_s.at[kind(s), kx - 1, km - 1], r1_r.at[s, kx - 1, km - 1], at_m(km))

    def relay_x(s, kx, km, ref):
        return copy(ref, ref, r2_s.at[kind(s), kx - 1, km - 1], r2_r.at[s, kx - 1, km - 1], at_x(kx))

    def across(s, kx, km, ref):
        return copy(ref, ref, p_s.at[kind(s)], p_r.at[s, km if is_up(s) else kx], partner)

    def issue_m(s):
        ref = block(s, 0, 0, c)
        for k in ms:
            direct_m(s, k, ref).start()
        if cores > 1:
            across(s, 0, 0, ref).start()

    def issue_x(s):
        ref = block(s, 0, 0, c)
        for k in xs:
            direct_x(s, k, ref).start()

    def issue(s):
        issue_m(s)
        issue_x(s)

    def forward_m(s):
        for km in ms:
            ref = block(s, 0, km, c)
            direct_m(s, km, ref).wait_recv()
            for k in xs:
                relay_x(s, k, km, block(s, 0, km, c, 1)).start()
            if cores > 1:
                across(s, 0, km, ref).start()

    def forward_x(s):
        for k in xs:
            ref = block(s, k, 0, c)
            direct_x(s, k, ref).wait_recv()
            for km in ms:
                relay_m(s, k, km, block(s, k, 0, c, 0)).start()
            if cores > 1:
                across(s, k, 0, ref).start()

    def collect(s, k):
        for km in ms:
            for part, relay in enumerate((relay_m, relay_x)):
                ref = block(s, k, km, c, part)
                relay(s, k, km, ref).wait_recv()
                if cores > 1:
                    across(s, k, km, ref).start()

    def take_up(s, km):
        if cores > 1:
            ref = upf.at[0, pl.ds(0, n_x * u_rows), :]
            across(s, 0, km, ref).wait_recv()

    def take(s, k):
        if cores > 1:
            ref = dn.at[(s - UP_STAGES) * n_x + x_from(k), :,
                        pl.ds(pl.multiple_of((cores - 1 - c) * LANES, LANES), LANES)]
            across(s, k, 0, ref).wait_recv()

    def own_down(j):
        return pltpu.make_async_copy(
            down_hbm.at[:, pl.ds(pl.multiple_of(j * LANES, LANES), LANES)],
            block(j + UP_STAGES, 0, 0, c), own_sem.at[j])

    def half(ref, h):
        return ref.at[pl.ds(h * (rows // 2), rows // 2), :]

    def token_up(e, h):
        src = xv if e == 0 else tok.at[g - e]
        return copy(half(src, h), half(tok.at[g - e], h), tu_s.at[e], tu_r.at[e, h], at_g(1))

    def token_down(e, h):
        src = xv if e == 0 else tok.at[g + e]
        return copy(half(src, h), half(tok.at[g + e], h), td_s.at[e], td_r.at[e, h], at_g(n_g - 1))

    def token_start(e):
        for h in range(2):
            @pl.when((g >= e) & (g < n_g - 1))
            def _():
                if e > 0:
                    ref = half(tok.at[g - e], h)
                    copy(ref, ref, tu_s.at[e], tu_r.at[e - 1, h], at_g(1)).wait_recv()
                token_up(e, h).start()

            @pl.when((g <= n_g - 1 - e) & (g > 0))
            def _():
                if e > 0:
                    ref = half(tok.at[g + e], h)
                    copy(ref, ref, td_s.at[e], td_r.at[e - 1, h], at_g(n_g - 1)).wait_recv()
                token_down(e, h).start()

    def token_end():
        for e in hops:
            for h in range(2):
                @pl.when((g >= e) & (g == n_g - 1))
                def _():
                    ref = half(tok.at[g - e], h)
                    copy(ref, ref, tu_s.at[0], tu_r.at[e - 1, h], at_g(1)).wait_recv()

                @pl.when((g <= n_g - 1 - e) & (g == 0))
                def _():
                    ref = half(tok.at[g + e], h)
                    copy(ref, ref, td_s.at[0], td_r.at[e - 1, h], at_g(n_g - 1)).wait_recv()

    def bias(k, src, slot):
        return copy(src, ubf.at[slot], bs_s.at[slot], bs_r.at[slot], at_m(k))

    def upward(v, e):
        part = pl.ds(e + 1, n_g - 1 - e)
        return copy(pb.at[v, part], from_low.at[v, part], lo_s.at[0], lo_r.at[v], at_g(1))

    def downward(v, e):
        part = pl.ds(0, n_g - 1 - e)
        return copy(pb.at[v, part], from_high.at[v, part], hi_s.at[0], hi_r.at[v], at_g(n_g - 1))

    def slab(d, h):
        if h is None:
            return d
        return d, pl.ds(h * (rows // 2), rows // 2)

    def piece_up(v, d, h):
        at = slab(d, h)
        at = (at,) if h is None else at
        return copy(pb.at[(v,) + at], from_low.at[(v,) + at], lo_s.at[0], end_r.at[0, v - v_tail, d if h != 1 else n_g], at_g(1))

    def piece_down(v, d, h):
        at = slab(d, h)
        at = (at,) if h is None else at
        return copy(pb.at[(v,) + at], from_high.at[(v,) + at], hi_s.at[0], end_r.at[1, v - v_tail, d if h != 1 else n_g],
                    at_g(n_g - 1))

    def normalize(values, at):
        values = values.astype(jnp.float32)
        center = jnp.mean(values, axis=1, keepdims=True)
        spread = jnp.mean((values - center) ** 2, axis=1, keepdims=True)
        lines = (values - center) * lax.rsqrt(spread + 1e-05) * gain[...] + nbias[...]
        normed[pl.ds(pl.multiple_of(at * rows, rows), rows), :] = lines.astype(jnp.bfloat16)

    barrier = pltpu.get_barrier_semaphore()
    near = [at_x(k) for k in xs] + [at_m(k) for k in ms]
    if cores > 1:
        near.append(partner)

    def greet(device):
        pl.semaphore_signal(barrier, inc=1, device_id=device, device_id_type=MESH)

    for device in near:
        greet(device)

    @pl.when(g < n_g - 1)
    def _():
        greet(at_g(1))

    @pl.when(g > 0)
    def _():
        greet(at_g(n_g - 1))

    own_up = upf.at[m, pl.ds(pl.multiple_of(img * depth, depth), depth), :]
    loads = [pltpu.make_async_copy(a, b, in_sem.at[i]) for i, (a, b) in enumerate((
        (x_hbm, xv), (up_hbm, own_up), (gain_hbm, gain), (nbias_hbm, nbias), (ubias_hbm, ubias), (dbias_hbm, dbias)))]
    for i in (1, 0, 2, 3, 4, 5):
        loads[i].start()
    loads[1].wait()
    ends = (g + n_g - 1) // n_g + (2 * n_g - 2 - g) // n_g
    pl.semaphore_wait(barrier, len(near) + ends)

    for s in range(UP_STAGES):
        issue(s)
    loads[0].wait()
    if n_g > 1:
        token_start(0)
    for j in range(n_chunk):
        own_down(j).start()
    for i in (2, 3, 4, 5):
        loads[i].wait()
    for k in ms:
        bias(k, ubias, k - 1).start()
    normalize(xv[...], g)

    def up_rows(km, first, last):
        place = lax.rem(m - km + pair, pair)
        biases = ubias if km == 0 else ubf.at[km - 1]

        def up_tile(n, carry):
            cols = pl.ds(pl.multiple_of(n * TILE, TILE), TILE)
            summed = jnp.dot(normed[...], upf[place, :, cols], preferred_element_type=jnp.float32)
            at = pl.ds(pl.multiple_of(place * units + n * TILE, TILE), TILE)
            hidden[:, at] = jax.nn.gelu(summed + biases[:, cols]).astype(jnp.bfloat16)
            return carry

        lax.fori_loop(first, last, up_tile, 0)

    for s in range(max(UP_STAGES, n_g - 1)):
        if 0 < s + 1 < n_g - 1:
            token_start(s + 1)
        if s < UP_STAGES:
            forward_m(s)
            forward_x(s)
    own_down(0).wait()
    issue(UP_STAGES)
    if n_chunk > 1:
        own_down(1).wait()
        issue_m(UP_STAGES + 1)
    token_end()
    for k in hops:
        o = lax.rem(g + k, n_g)
        normalize(tok[o], o)
    for s in range(UP_STAGES):
        take_up(s, 0)
    up_rows(0, 0, n_tile)
    for s in range(UP_STAGES):
        for k in xs:
            collect(s, k)
    for km in ms:
        bias(km, ubias, km - 1).wait_recv()
        for s in range(UP_STAGES):
            take_up(s, km)
        up_rows(km, 0, n_tile // 2)
        if km == pair - 1:
            forward_m(UP_STAGES)
            if n_chunk > 1:
                issue_x(UP_STAGES + 1)
        up_rows(km, n_tile // 2, n_tile)
    if pair == 1 and n_chunk > 1:
        issue_x(UP_STAGES + 1)

    def multiply(v, j, k):
        value = jnp.dot(hidden[...], dn[j * n_x + x_from(k)], preferred_element_type=jnp.float32)
        pb[v] = value.reshape(n_g, rows, wide).astype(jnp.bfloat16)

    upper = 2 * g // n_g
    far_d = (1 - upper) * (n_g - 1)

    def multiply_far(v, j, k):
        lines = hidden[pl.ds(pl.multiple_of(far_d * rows, rows), rows), :]
        value = jnp.dot(lines, dn[j * n_x + x_from(k)], preferred_element_type=jnp.float32)
        pb[v, far_d] = value.astype(jnp.bfloat16)

    def multiply_rest(v, j, k):
        if n_g > 1:
            lines = hidden[pl.ds(pl.multiple_of(upper * rows, rows), (n_g - 1) * rows), :]
            value = jnp.dot(lines, dn[j * n_x + x_from(k)], preferred_element_type=jnp.float32)
            pb[v, pl.ds(upper, n_g - 1)] = value.reshape(n_g - 1, rows, wide).astype(jnp.bfloat16)

    def add(v, part, arrived):
        at = (v,) + part if isinstance(part, tuple) else (v, part)
        pb[at] = (pb[at].astype(jnp.float32) + arrived[at].astype(jnp.float32)).astype(jnp.bfloat16)

    def pass_on(step):
        for e in reversed(range(n_g - 1)):
            v = step - LAG * e

            @pl.when((g == e) & (v >= 0) & (v < v_tail))
            def _():
                if e > 0:
                    upward(v, e - 1).wait_recv()
                    add(v, pl.ds(e + 1, n_g - 1 - e), from_low)
                upward(v, e).start()

            @pl.when((g == n_g - 1 - e) & (v >= 0) & (v < v_tail))
            def _():
                if e > 0:
                    downward(v, e - 1).wait_recv()
                    add(v, pl.ds(0, n_g - 1 - e), from_high)
                downward(v, e).start()

    def pass_pieces(step, first, stop):
        for e in reversed(range(n_g - 1)):
            v = step - LAG * e
            for i in range(first, min(stop, n_g - 1 - e)):
                for here, d, piece, arrived in (
                        (e, n_g - 1 - i, piece_up, from_low), (n_g - 1 - e, i, piece_down, from_high)):
                    @pl.when((g == here) & (v >= v_tail) & (v < n_v))
                    def _():
                        for h in (0, 1) if i == 0 else (None,):
                            if e > 0:
                                piece(v, d, h).wait_recv()
                                add(v, slab(d, h), arrived)
                            piece(v, d, h).start()

    def pass_far(step):
        pass_on(step)
        pass_pieces(step, 0, 1)

    def pass_near(step):
        pass_pieces(step, 1, n_g)

    def reduce(v):
        some = (v + n_v - 1) // n_v
        i = (v + n_x - 1) // n_x
        k = lax.rem(v + n_x - 1, n_x) * some + i // n_chunk
        j = i - (k + n_x - 1) // n_x
        for d in range(n_g):
            @pl.when(g == d)
            def _():
                if isinstance(v, int) and v >= v_tail:
                    if d > 0:
                        for h in (0, 1) if d == n_g - 1 else (None,):
                            piece_up(v, d, h).wait_recv()
                    if d < n_g - 1:
                        for h in (0, 1) if d == 0 else (None,):
                            piece_down(v, d, h).wait_recv()
                elif n_g > 1:
                    if d == n_g - 1:
                        upward(v, d - 1).wait_recv()
                    if d == 0:
                        downward(v, n_g - 2).wait_recv()

        src_x = x_from(k)
        for core in range(cores):
            cols = pl.ds(pl.multiple_of(((src_x * cores + core) * n_chunk + j) * LANES, LANES), LANES)
            piece = slice(core * LANES, (core + 1) * LANES)
            total = pb[v, g, :, piece].astype(jnp.float32) + dbias[:, cols]
            below = from_low[v, g, :, piece].astype(jnp.float32)
            above = from_high[v, g, :, piece].astype(jnp.float32)
            total = total + jnp.where(g > 0, below, 0.0) + jnp.where(g < n_g - 1, above, 0.0)
            out_ref[:, cols] = total.astype(jnp.bfloat16)

    settle = LAG * (n_g - 1) + 1

    def settled(v):
        @pl.when(v >= settle)
        def _():
            reduce(v - settle)

    def unit(v, j, k):
        take(j + UP_STAGES, k)
        multiply(v, j, k)
        pass_far(v)

        @pl.when(v < n_v - 2)
        def _():
            pass_near(v)

        settled(v)

    def last_unit(j, k):
        take(j + UP_STAGES, k)
        multiply_far(v_last, j, k)
        pass_far(v_last)
        multiply_rest(v_last, j, k)
        settled(v_last)

    def later(i, base, stop):
        def one(k, carry):
            collect(i + UP_STAGES, k)
            unit(base + k, i, k)
            return carry

        lax.fori_loop(1, stop, one, 0)

    def start(i):
        @pl.when(i + 2 < n_chunk)
        def _():
            own_down(i + 2).wait()
            issue(i + 2 + UP_STAGES)

    def tick(i, carry):
        forward_m(i + UP_STAGES)
        forward_x(i + UP_STAGES)
        start(i)
        unit(n_x * (i - 1) + 1, i, 0)
        later(i - 1, n_x * (i - 1) + 1, n_x)
        return carry

    unit(0, 0, 0)
    forward_x(UP_STAGES)
    start(0)
    if n_x > 1 and n_chunk > 1:
        forward_m(1 + UP_STAGES)
        unit(1, 1, 0)
        for k in xs:
            collect(UP_STAGES, k)
        forward_x(1 + UP_STAGES)
        start(1)
        for k in xs:
            unit(1 + k, 0, k)
        lax.fori_loop(2, n_chunk, tick, 0)
        later(n_chunk - 1, n_x * (n_chunk - 1), n_x - 1)
        collect(n_chunk - 1 + UP_STAGES, n_x - 1)
        last_unit(n_chunk - 1, n_x - 1)
    else:
        lax.fori_loop(1, n_chunk - 1, tick, 0)
        forward_m(n_chunk - 1 + UP_STAGES)
        forward_x(n_chunk - 1 + UP_STAGES)
        last_unit(n_chunk - 1, 0)

    def drain(step, carry):
        pass_far(step)
        pass_near(step - 2)
        return carry

    def reduce_tick(v, carry):
        reduce(v)
        return carry

    lax.fori_loop(n_v, n_v + LAG * (n_g - 2) + 2, drain, 0)
    lax.fori_loop(max(n_v - settle, 0), v_tail, reduce_tick, 0)
    for v in range(v_tail, n_v):
        reduce(v)

    for t in range(2):
        s = 0 if t == 0 else UP_STAGES
        cut = low_part[t]

        def span(size):
            if t == 0:
                return upf.at[0, pl.ds(0, UP_STAGES * size), :]
            return dn.at[pl.ds(0, n_chunk), pl.ds(0, size), pl.ds(0, LANES)]

        full = u_rows if t == 0 else units
        for k in xs:
            direct_x(s, k, span(full)).wait_send()
        for k in ms:
            direct_m(s, k, span(full)).wait_send()
        for k in xs:
            for km in ms:
                relay_m(s, k, km, span(cut)).wait_send()
                relay_x(s, k, km, span(full - cut)).wait_send()
        if cores > 1:
            ref = upf.at[:, pl.ds(0, n_x * depth), :] if t == 0 else dn.at[:, :, pl.ds(0, LANES)]
            across(s, 0, 0, ref).wait_send()
    for e in range(n_g - 1):
        @pl.when(g == e)
        def _():
            ref = pb.at[:, pl.ds(e + 1, n_g - 1 - e)]
            copy(ref, ref, lo_s.at[0], lo_r.at[0], at_g(1)).wait_send()

        @pl.when(g == n_g - 1 - e)
        def _():
            ref = pb.at[:, pl.ds(0, n_g - 1 - e)]
            copy(ref, ref, hi_s.at[0], hi_r.at[0], at_g(n_g - 1)).wait_send()
    for e in range(n_g - 1):
        @pl.when((g >= e) & (g < n_g - 1))
        def _():
            copy(tok.at[0], tok.at[0], tu_s.at[e], tu_r.at[e, 0], at_g(1)).wait_send()

        @pl.when((g <= n_g - 1 - e) & (g > 0))
        def _():
            copy(tok.at[0], tok.at[0], td_s.at[e], td_r.at[e, 0], at_g(n_g - 1)).wait_send()
    for k in ms:
        bias(k, ubias, k - 1).wait_send()


def solution(mesh):
    n_img, n_tp = mesh.shape["img"], mesh.shape["tp"]
    cores = 2 if n_img % 2 == 0 else 1
    pair = 2 if n_tp % 2 == 0 else 1
    n_x, n_g = n_img // cores, n_tp // pair

    def on_device(x, gain, nbias, up, ubias, down, dbias):
        rows, width = x.shape
        depth, units = up.shape
        n_chunk = down.shape[1] // LANES
        stages = UP_STAGES + n_chunk
        n_v, wide = n_chunk * n_x, cores * LANES
        out_width = n_img * down.shape[1]
        bf16, f32 = jnp.bfloat16, jnp.float32
        dma = pltpu.SemaphoreType.DMA
        ox, om, og = max(n_x - 1, 1), max(pair - 1, 1), max(n_g - 1, 1)
        scratch = [
            pltpu.VMEM((rows, width), bf16),
            pltpu.VMEM((1, width), f32),
            pltpu.VMEM((1, width), f32),
            pltpu.VMEM((1, units), f32),
            pltpu.VMEM((1, out_width), f32),
            pltpu.VMEM((n_g, rows, width), bf16),
            pltpu.VMEM((n_g * rows, width), bf16),
            pltpu.VMEM((pair, width, units), bf16),
            pltpu.VMEM((om, 1, units), f32),
            pltpu.VMEM((n_g * rows, pair * units), bf16),
            pltpu.VMEM((n_v, pair * units, wide), bf16),
            pltpu.VMEM((n_v, n_g, rows, wide), bf16),
            pltpu.VMEM((n_v, n_g, rows, wide), bf16),
            pltpu.VMEM((n_v, n_g, rows, wide), bf16),
        ]
        scratch += [dma((6,)), dma((n_chunk,))]
        scratch += [dma((og,)), dma((og, 2))] * 2 + [dma((om,))] * 2
        scratch += [dma((2, ox)), dma((stages, ox)), dma((2, om)), dma((stages, om))]
        scratch += [dma((2, ox, om)), dma((stages, ox, om))] * 2
        scratch += [dma((2,)), dma((stages, max(n_x, pair)))]
        scratch += [dma((1,)), dma((max(n_v - TAIL, 1),))] * 2 + [dma((2, TAIL, n_g + 1))]
        return pl.pallas_call(
            functools.partial(kernel, n_img, n_tp),
            out_shape=pltpu.VMEM((rows, out_width), bf16),
            in_specs=[pl.BlockSpec(memory_space=pl.ANY)] * 7,
            out_specs=pl.BlockSpec(memory_space=pltpu.VMEM),
            scratch_shapes=scratch,
            compiler_params=pltpu.CompilerParams(
                collective_id=0, has_side_effects=True, vmem_limit_bytes=60 * 1024 * 1024),
        )(x, gain.reshape(1, -1), nbias.reshape(1, -1), up, ubias.reshape(1, -1), down,
          dbias.reshape(1, -1))

    return jax.shard_map(
        on_device,
        mesh=mesh,
        in_specs=(P(("img", "tp"), None), P(), P(), P("img", "tp"), P("tp"), P("tp", "img"), P()),
        out_specs=P(("img", "tp"), None),
        check_vma=False,
    )
```
